256 devices in a mesh: seq: 128 (over x, z_lo, y, core), head: 2 (over z_hi).
Axes of the slice: x: 4, y: 4, z: 8 (z_hi: 2, z_lo: 4; z = z_hi * 4 + z_lo), core: 2. Of those that a mesh axis runs over, the one named last changes fastest.
Arguments:
- queries: bfloat16 [16384, 2048], P('seq', 'head'), may hold values from -6 to 6
- keys: bfloat16 [16384, 512], P('seq', 'head'), may hold values from -6 to 6
- values: bfloat16 [16384, 512], P('seq', 'head'), may hold values from -6 to 6
- tile_mask: int32 [256, 256], replicated, may hold values from 0 to 1, as said below
- out_weight: bfloat16 [2048, 4096], P('head'), may hold values from -0.5 to 0.5
Outputs:
- mixed: bfloat16 [16384, 4096], P(('seq', 'head'))
The draws below stay inside these ranges and needn't reach their ends.
Inputs may be any that keep to these rules, and one draw needn't show every extreme that they name: tile_mask[i, j] is 1 for i == j, 0 for j > i, and 0 or 1 below the diagonal.
All inputs are finite; a program needn't handle non-finite values.
Results may differ from the reference program's by a relative error of at most 0.01.
Values may be sent and summed in bfloat16 or wider, within the bound.
A program may use at most 128 MiB of HBM per device.

```python
import math
import jax
import jax.numpy as jnp
from jax import lax

D = 4096
HD = 128
HEADS = 16
KVH = 4
TILE = 64
TOKENS = 16384
TILES = 256


def draw_field(key, salt, heads_count):
    base = jax.random.fold_in(key, salt)
    field = 1.5 * jax.random.truncated_normal(base, -4.0, 4.0, (TOKENS, heads_count * HD), jnp.float32)
    return field.astype(jnp.bfloat16)


def draw_queries(key, part):
    return draw_field(key, 1, HEADS)


def draw_keys(key, part):
    return draw_field(key, 2, KVH)


def draw_tile_mask(key, part):
    coin = jax.random.randint(jax.random.fold_in(key, 3), (TILES, TILES), 0, 2, dtype=jnp.int32)
    row_index = jnp.arange(TILES, dtype=jnp.int32)[:, None]
    column_index = jnp.arange(TILES, dtype=jnp.int32)[None, :]
    diagonal = jnp.where(row_index == column_index, 1, 0).astype(jnp.int32)
    return jnp.where(row_index > column_index, coin, diagonal).astype(jnp.int32)


def level_of(stream_key, dims, split, low, top_value):
    def one(axis_at, shards_of):
        heights = jax.random.uniform(jax.random.fold_in(jax.random.fold_in(stream_key, 6), axis_at), (shards_of,), jnp.float32, low / len(split), top_value / len(split))
        return jnp.repeat(jnp.exp(heights), dims[axis_at] // shards_of).reshape((-1,) + (1,) * (len(dims) - axis_at - 1))

    gain = one(*split[0])
    for cut in split[1:]:
        gain = gain * one(*cut)
    return gain


def scatter_about(stream_key, dims, deviation, reach, split=(), kind=jnp.bfloat16):
    result = deviation * jax.random.normal(stream_key, dims, jnp.float32)
    if split:
        result = result * level_of(stream_key, dims, split, -0.22, 0.18)
    return jnp.clip(result, -reach, reach).astype(kind)


def setup_inputs(seed: int = 0) -> dict:
    key_of = jax.random.split(jax.random.key(seed), 6)
    return {
        "queries": draw_queries(jax.random.fold_in(key_of[5], 71), 0),
        "keys": draw_keys(jax.random.fold_in(key_of[5], 71), 0),
        "values": scatter_about(key_of[2], (TOKENS, KVH * HD), 1.0, 6.0, ((0, 128), (1, 2))),
        "tile_mask": draw_tile_mask(jax.random.fold_in(key_of[5], 71), 0),
        "out_weight": scatter_about(key_of[4], (HEADS * HD, D), HD ** -0.5, 0.5, ((0, 2),)),
    }


MASK_FLOOR = -1e+30

def reference(queries, keys, values, tile_mask, out_weight):
    group = HEADS // KVH
    scale = 1.0 / math.sqrt(HD)
    query_field = queries.reshape(TOKENS, KVH, group, HD)
    key_field = keys.reshape(TOKENS, KVH, HD).astype(jnp.float32)
    value_field = values.reshape(TOKENS, KVH, HD).astype(jnp.float32)
    key_index = jnp.arange(TOKENS, dtype=jnp.int32)
    key_tile = key_index // TILE

    def one_tile(tile):
        row_start = (tile * TILE).astype(jnp.int32)
        query_tile = lax.dynamic_slice_in_dim(query_field, row_start, TILE, 0).astype(jnp.float32)
        query_index = row_start + jnp.arange(TILE, dtype=jnp.int32)
        mask_row = lax.dynamic_index_in_dim(tile_mask, tile, 0, keepdims=False)
        allowed = (mask_row[key_tile] > 0)[None, :] & (key_index[None, :] <= query_index[:, None])
        allowed_wide = allowed[:, None, None, :]
        scores = jnp.einsum('qgrd,kgd->qgrk', query_tile, key_field, precision=lax.Precision.HIGHEST) * scale
        masked = jnp.where(allowed_wide, scores, MASK_FLOOR)
        best = lax.optimization_barrier(jnp.max(masked, axis=-1, keepdims=True))
        weights = jnp.where(allowed_wide, jnp.exp(masked - best), 0.0)
        total = lax.optimization_barrier(jnp.sum(weights, axis=-1))
        rounded = lax.optimization_barrier(weights.astype(jnp.bfloat16)).astype(jnp.float32)
        blended = jnp.einsum('qgrk,kgd->qgrd', rounded, value_field, precision=lax.Precision.HIGHEST) / total[..., None]
        return blended.astype(jnp.bfloat16).reshape(TILE, HEADS * HD)
    attended = lax.map(one_tile, jnp.arange(TILES, dtype=jnp.int32)).reshape(TOKENS, HEADS * HD)
    return jnp.dot(attended, out_weight, preferred_element_type=jnp.float32).astype(jnp.bfloat16)
```

```python
import math

import jax
import jax.numpy as jnp
from jax import lax
from jax.experimental import pallas as pl
from jax.experimental.pallas import tpu as pltpu
from jax.sharding import PartitionSpec as P

HD = 128
MESH = pl.DeviceIdType.MESH
OFF = -1e30
FLOOR = -1e6
EXP_SCALE = math.log2(math.e) / math.sqrt(HD)
COLS = 512


def kernel(q_hbm, k_hbm, v_hbm, mask_hbm, w_hbm, out_ref,
           buf, qs, w, mask8, bias, dbias, mx, ls, acc, att, osend, pown, psend, precv,
           lsem, qlsem, wsem, msem, zs, zr, qss, qsr, a_s, a_r, b_s, b_r, d_s, d_r, o_s, o_r, p_s, p_r):
    s = lax.axis_index("seq")
    h = lax.axis_index("head")
    c = s % 2
    y = (s // 2) % 4
    z = (s // 8) % 4
    x = s // 32
    a = y * (1 - c) + x * c
    b = x * (1 - c) + y * c
    g = z % 2
    chip = x * 16 + z * 4 + y
    pair_z = z + 1 - 2 * g
    pair_chip = (3 - x) * 16 + pair_z * 4 + y

    def dev(xx, zz, yy, cc, hh):
        return {"seq": ((xx * 4 + zz) * 4 + yy) * 2 + cc, "head": hh}

    def a_dev(d):
        return dev((x + c * d + 4) % 4, z, (y + (1 - c) * d + 4) % 4, c, h)

    def b_dev(d):
        return dev((x + (1 - c) * d + 4) % 4, z, (y + c * d + 4) % 4, c, h)

    def z_of(k):
        return ((z // 2 + k // 2) % 2) * 2 + (z % 2 + k % 2) % 2

    mate = dev(x, z, y, 1 - c, h)
    pair = dev(3 - x, pair_z, y, c, h)
    across = dev(x, z, y, c, 1 - h)

    def remote(src, dst, ss, rs, to):
        return pltpu.make_async_remote_copy(
            src_ref=src, dst_ref=dst, send_sem=ss, recv_sem=rs, device_id=to, device_id_type=MESH)

    def cols(start, size):
        return pl.ds(pl.multiple_of(start, 128), size)

    locals_ = [
        pltpu.make_async_copy(k_hbm.at[:, cols(g * 128, 128)], buf.at[c, b, z, 0, a], lsem.at[0]),
        pltpu.make_async_copy(v_hbm.at[:, cols(g * 128, 128)], buf.at[c, b, z, 1, a], lsem.at[1]),
    ]
    qlocals = [
        pltpu.make_async_copy(q_hbm.at[:, cols(g * 512 + i * 128, 128)], qs.at[0, i], qlsem.at[i])
        for i in range(4)
    ]
    mask_own = pltpu.make_async_copy(
        mask_hbm.at[pl.ds(pl.multiple_of((chip // 2) * 8, 8), 8)], mask8.at[0], msem.at[0])
    mask_pair = pltpu.make_async_copy(
        mask_hbm.at[pl.ds(pl.multiple_of((pair_chip // 2) * 8, 8), 8)], mask8.at[1], msem.at[1])
    for cp in locals_:
        cp.start()

    barrier = pltpu.get_barrier_semaphore()
    friends = [a_dev(1), a_dev(-1), b_dev(1), b_dev(-1), mate, pair, across] + [
        dev(x, z_of(k), y, c, h) for k in (1, 2, 3)]
    for f in friends:
        pl.semaphore_signal(barrier, inc=1, device_id=f, device_id_type=MESH)
    mask_own.start()
    mask_pair.start()
    for cp in qlocals:
        cp.start()
    pl.semaphore_wait(barrier, len(friends))

    def z_copy(k, t):
        src = k_hbm if t == 0 else v_hbm
        zt = z_of(k)
        return remote(src.at[:, cols((zt % 2) * 128, 128)], buf.at[c, b, z, t, a],
                      zs.at[k, t], zr.at[k, t], dev(x, zt, y, c, h))

    def q_copy(i):
        return remote(q_hbm.at[:, cols((1 - g) * 512 + i * 128, 128)], qs.at[1, i],
                      qss.at[i], qsr.at[i], pair)

    def a_copy(k, way):
        zt = z_of(k)
        if way == 0:
            ref, to = buf.at[c, b, zt, :, a], a_dev(1)
        elif way == 1:
            ref, to = buf.at[c, b, zt, :, a], a_dev(-1)
        elif way == 2:
            ref, to = buf.at[c, b, zt, 0, (a + 3) % 4], a_dev(1)
        else:
            ref, to = buf.at[c, b, zt, 1, (a + 1) % 4], a_dev(-1)
        return remote(ref, ref, a_s.at[k, way], a_r.at[k, way], to)

    def b_copy(k, way):
        zt = z_of(k)
        if way == 0:
            ref, to = buf.at[c, b, zt], b_dev(1)
        elif way == 1:
            ref, to = buf.at[c, b, zt], b_dev(-1)
        elif way == 2:
            ref, to = buf.at[c, (b + 3) % 4, zt, 0], b_dev(1)
        else:
            ref, to = buf.at[c, (b + 1) % 4, zt, 1], b_dev(-1)
        return remote(ref, ref, b_s.at[k, way], b_r.at[k, way], to)

    def unit_of(base, i):
        return (base + (4 - i) * (i % 2) * (1 - i // 2) + (i // 2) * (1 + i % 2)) % 4

    def d_copy(k, i):
        ref = buf.at[c, unit_of(b, i), z_of(k)]
        return remote(ref, ref, d_s.at[k, i], d_r.at[k, i], mate)

    for k in (1, 2, 3):
        for t in range(2):
            z_copy(k, t).start()
    for i in range(4):
        q_copy(i).start()
    for cp in locals_:
        cp.wait()
    a_copy(0, 0).start()
    a_copy(0, 1).start()
    wcopy = pltpu.make_async_copy(w_hbm, w, wsem)
    wcopy.start()

    mask_own.wait()
    mask_pair.wait()
    lane = lax.broadcasted_iota(jnp.int32, (8, 128), 1)
    for r, row_chip in ((0, chip), (1, pair_chip)):
        at = (row_chip % 2) * 2 + c
        all8 = mask8[r]
        two = jnp.where(at < 2, jnp.where(at == 0, all8[0:2], all8[2:4]),
                        jnp.where(at == 2, all8[4:6], all8[6:8]))
        rows8 = jnp.concatenate([two] * 4, axis=0)
        open8 = jnp.where(rows8 > 0, 0.0, OFF).astype(jnp.float32)
        for blk in range(128):
            first = jnp.broadcast_to(open8[:, 2 * blk:2 * blk + 1], (8, 128))
            second = jnp.broadcast_to(open8[:, 2 * blk + 1:2 * blk + 2], (8, 128))
            bias[r, blk] = jnp.where(lane < 64, first, second)
        own_blk = row_chip * 2 + c
        dbias[r] = bias[r, own_blk]
        bias[r, own_blk] = jnp.full((8, 128), OFF, jnp.float32)

    mx[...] = jnp.full(mx.shape, FLOOR, jnp.float32)
    ls[...] = jnp.zeros(ls.shape, jnp.float32)
    acc[...] = jnp.zeros(acc.shape, jnp.float32)

    def update(r, scores, vals):
        old = mx[r]
        best = jnp.max(scores, axis=1, keepdims=True)
        new = jnp.maximum(old, best)
        probs = jnp.exp2((scores - new[:, :1]) * EXP_SCALE)
        shrink = jnp.exp2((old - new) * EXP_SCALE)
        part = probs[:, 0:128]
        for j in range(1, probs.shape[1] // 128):
            part = part + probs[:, j * 128:(j + 1) * 128]
        ls[r] = ls[r] * shrink + part
        acc[r] = acc[r] * shrink + jnp.dot(
            probs.astype(jnp.bfloat16), vals, preferred_element_type=jnp.float32)
        mx[r] = new

    def spread(rows):
        two = [jnp.broadcast_to(rows[t:t + 1], (64, rows.shape[1])) for t in range(2)]
        one = jnp.concatenate(two, axis=0)
        return jnp.concatenate([one] * 4, axis=0)

    def attend(st, bb, zz, r):
        low_chip = (1 - st) * (bb * 16 + zz * 4) + st * (zz * 4 + bb)
        row_chip = chip * (1 - r) + pair_chip * r

        @pl.when(low_chip <= row_chip)
        def _():
            keys = buf[st, bb, zz, 0].reshape(512, HD)
            vals = buf[st, bb, zz, 1].reshape(512, HD)
            scores = lax.dot_general(qs[r].reshape(512, HD), keys, (((1,), (1,)), ((), ())),
                                     preferred_element_type=jnp.float32)
            rows = []
            for i in range(4):
                at = ((1 - st) * (bb * 16 + zz * 4 + i) + st * (i * 16 + zz * 4 + bb)) * 2 + st
                rows.append(bias[r, at][0:2])
            update(r, scores + spread(jnp.concatenate(rows, axis=1)), vals)

    def diagonal(r, carry):
        zz = z * (1 - r) + pair_z * r
        xx = x * (1 - r) + (3 - x) * r
        aa = y * (1 - c) + xx * c
        bb = xx * (1 - c) + y * c
        keys = buf[c, bb, zz, 0, aa]
        vals = buf[c, bb, zz, 1, aa]
        scores = lax.dot_general(qs[r].reshape(512, HD), keys, (((1,), (1,)), ((), ())),
                                 preferred_element_type=jnp.float32)
        row = lax.broadcasted_iota(jnp.int32, (512, 128), 0) % 128
        col = lax.broadcasted_iota(jnp.int32, (512, 128), 1)
        rows = dbias[r][0:2]
        scores = jnp.where(col <= row, scores + spread(rows), OFF)
        update(r, scores, vals)
        return carry

    def stream_units(k, first, count):
        def body(t, carry):
            other = t // (2 * count)
            i = first + (t // 2) % count
            r = t % 2

            @pl.when((other == 1) & (r == 0))
            def _():
                d_copy(k, i).wait_recv()

            st = c * (1 - other) + (1 - c) * other
            base = b * (1 - other) + a * other
            attend(st, unit_of(base, i), z_of(k), r)
            return carry

        lax.fori_loop(0, 4 * count, body, 0)

    def a_forward(k):
        a_copy(k, 0).wait_recv()
        a_copy(k, 2).start()
        a_copy(k, 1).wait_recv()
        a_copy(k, 3).start()

    def a_begin(k):
        z_copy(k, 0).wait_recv()
        z_copy(k, 1).wait_recv()
        a_copy(k, 0).start()
        a_copy(k, 1).start()

    def b_begin(k):
        a_copy(k, 2).wait_recv()
        a_copy(k, 3).wait_recv()
        b_copy(k, 0).start()
        b_copy(k, 1).start()
        d_copy(k, 0).start()

    a_forward(0)
    a_begin(1)
    b_begin(0)
    a_forward(1)
    a_begin(2)
    b_begin(1)
    a_forward(2)
    a_begin(3)
    b_begin(2)
    a_forward(3)
    b_begin(3)
    for cp in qlocals:
        cp.wait()
    for i in range(4):
        q_copy(i).wait()

    def own_units(k, carry):
        stream_units(k, 0, 1)
        return carry

    lax.fori_loop(0, 4, own_units, 0)

    def near_units(k, carry):
        b_copy(k, 0).wait_recv()
        b_copy(k, 2).start()
        b_copy(k, 1).wait_recv()
        b_copy(k, 3).start()
        d_copy(k, 1).start()
        d_copy(k, 2).start()
        stream_units(k, 1, 2)
        return carry

    lax.fori_loop(0, 4, near_units, 0)
    lax.fori_loop(0, 2, diagonal, 0)

    def far_units(k, carry):
        b_copy(k, 2).wait_recv()
        b_copy(k, 3).wait_recv()
        d_copy(k, 3).start()
        stream_units(k, 3, 1)
        return carry

    lax.fori_loop(0, 4, far_units, 0)

    def result(r):
        total = jnp.sum(ls[r], axis=1, keepdims=True)
        done = (acc[r] / total).astype(jnp.bfloat16)
        return jnp.concatenate([done[i * 128:(i + 1) * 128] for i in range(4)], axis=1)

    osend[...] = result(1)
    o_copy = remote(osend, att.at[g], o_s, o_r, pair)
    o_copy.start()
    att[g] = result(0)
    wcopy.wait()
    o_copy.wait()

    def p_copy(n):
        return remote(psend.at[n], precv.at[n], p_s.at[n], p_r.at[n], across)

    def project(n, carry):
        at = cols(n * COLS, COLS)
        part = jnp.dot(att[0], w[0:512, at], preferred_element_type=jnp.float32)
        part = part + jnp.dot(att[1], w[512:1024, at], preferred_element_type=jnp.float32)
        upper, lower = part[0:64], part[64:128]
        mine = jnp.where(h == 0, upper, lower)
        theirs = jnp.where(h == 0, lower, upper)
        psend[n] = theirs.astype(jnp.bfloat16)
        p_copy(n).start()
        pown[n] = mine
        return carry

    lax.fori_loop(0, 4096 // COLS, project, 0)

    def finish(n, carry):
        p_copy(n).wait()
        out_ref[:, cols(n * COLS, COLS)] = (pown[n] + precv[n].astype(jnp.float32)).astype(jnp.bfloat16)
        return carry

    lax.fori_loop(0, 4096 // COLS, finish, 0)

    def drain(k, carry):
        for way in range(4):
            a_copy(k, way).wait_send()
            b_copy(k, way).wait_send()
        for i in range(4):
            d_copy(k, i).wait_send()
        return carry

    lax.fori_loop(0, 4, drain, 0)
    for k in (1, 2, 3):
        for t in range(2):
            z_copy(k, t).wait_send()


def per_device(queries, keys, values, tile_mask, out_weight):
    dma = pltpu.SemaphoreType.DMA
    bf, f32 = jnp.bfloat16, jnp.float32
    n = 4096 // COLS
    return pl.pallas_call(
        kernel,
        out_shape=jax.ShapeDtypeStruct((64, 4096), bf),
        in_specs=[pl.BlockSpec(memory_space=pltpu.HBM)] * 5,
        out_specs=pl.BlockSpec(memory_space=pltpu.VMEM),
        scratch_shapes=[
            pltpu.VMEM((2, 4, 4, 2, 4, 128, 128), bf),
            pltpu.VMEM((2, 4, 128, 128), bf),
            pltpu.VMEM((1024, 4096), bf),
            pltpu.VMEM((2, 8, 256), jnp.int32),
            pltpu.VMEM((2, 128, 8, 128), f32),
            pltpu.VMEM((2, 8, 128), f32),
            pltpu.VMEM((2, 512, 128), f32),
            pltpu.VMEM((2, 512, 128), f32),
            pltpu.VMEM((2, 512, 128), f32),
            pltpu.VMEM((2, 128, 512), bf),
            pltpu.VMEM((128, 512), bf),
            pltpu.VMEM((n, 64, COLS), f32),
            pltpu.VMEM((n, 64, COLS), bf),
            pltpu.VMEM((n, 64, COLS), bf),
            dma((2,)), dma((4,)), dma, dma((2,)),
            dma((4, 2)), dma((4, 2)), dma((4,)), dma((4,)),
            dma((4, 4)), dma((4, 4)), dma((4, 4)), dma((4, 4)), dma((4, 4)), dma((4, 4)),
            dma, dma, dma((n,)), dma((n,)),
        ],
        compiler_params=pltpu.CompilerParams(
            collective_id=0, has_side_effects=True, vmem_limit_bytes=48 * 1024 * 1024),
    )(queries, keys, values, tile_mask, out_weight)


def solution(mesh):
    placed = (P("seq", "head"), P("seq", "head"), P("seq", "head"), P(), P("head", None))
    return jax.shard_map(
        per_device, mesh=mesh, in_specs=placed, out_specs=P(("seq", "head"), None), check_vma=False
    )
```

```python
import math

import jax
import jax.numpy as jnp
from jax import lax
from jax.experimental import pallas as pl
from jax.experimental.pallas import tpu as pltpu
from jax.sharding import PartitionSpec as P

HD = 128
MESH = pl.DeviceIdType.MESH
OFF = -1e30
FLOOR = -1e6
EXP_SCALE = math.log2(math.e) / math.sqrt(HD)
COLS = 512


def kernel(q_hbm, k_hbm, v_hbm, mask_hbm, w_hbm, out_ref,
           buf, qs, w, mask8, bias, dbias, mx, ls, acc, sbuf, att, osend, pown, psend, precv,
           lsem, qlsem, wsem, msem, zs, zr, qss, qsr, a_s, a_r, b_s, b_r, d_s, d_r, o_s, o_r, p_s, p_r):
    s = lax.axis_index("seq")
    h = lax.axis_index("head")
    c = s % 2
    y = (s // 2) % 4
    z = (s // 8) % 4
    x = s // 32
    a = y * (1 - c) + x * c
    b = x * (1 - c) + y * c
    g = z % 2
    chip = x * 16 + z * 4 + y
    pair_z = z + 1 - 2 * g
    pair_chip = (3 - x) * 16 + pair_z * 4 + y

    def dev(xx, zz, yy, cc, hh):
        return {"seq": ((xx * 4 + zz) * 4 + yy) * 2 + cc, "head": hh}

    def a_dev(d):
        return dev((x + c * d + 4) % 4, z, (y + (1 - c) * d + 4) % 4, c, h)

    def b_dev(d):
        return dev((x + (1 - c) * d + 4) % 4, z, (y + c * d + 4) % 4, c, h)

    def z_of(k):
        return ((z // 2 + k // 2) % 2) * 2 + (z % 2 + k % 2) % 2

    mate = dev(x, z, y, 1 - c, h)
    pair = dev(3 - x, pair_z, y, c, h)
    across = dev(x, z, y, c, 1 - h)

    def remote(src, dst, ss, rs, to):
        return pltpu.make_async_remote_copy(
            src_ref=src, dst_ref=dst, send_sem=ss, recv_sem=rs, device_id=to, device_id_type=MESH)

    def cols(start, size):
        return pl.ds(pl.multiple_of(start, 128), size)

    locals_ = [
        pltpu.make_async_copy(k_hbm.at[:, cols(g * 128, 128)], buf.at[c, b, z, 0, a], lsem.at[0]),
        pltpu.make_async_copy(v_hbm.at[:, cols(g * 128, 128)], buf.at[c, b, z, 1, a], lsem.at[1]),
    ]
    qlocals = [
        pltpu.make_async_copy(q_hbm.at[:, cols(g * 512 + i * 128, 128)], qs.at[0, i], qlsem.at[i])
        for i in range(4)
    ]
    mask_own = pltpu.make_async_copy(
        mask_hbm.at[pl.ds(pl.multiple_of((chip // 2) * 8, 8), 8)], mask8.at[0], msem.at[0])
    mask_pair = pltpu.make_async_copy(
        mask_hbm.at[pl.ds(pl.multiple_of((pair_chip // 2) * 8, 8), 8)], mask8.at[1], msem.at[1])
    for cp in locals_:
        cp.start()

    barrier = pltpu.get_barrier_semaphore()
    friends = [a_dev(1), a_dev(-1), b_dev(1), b_dev(-1), mate, pair, across] + [
        dev(x, z_of(k), y, c, h) for k in (1, 2, 3)]
    for f in friends:
        pl.semaphore_signal(barrier, inc=1, device_id=f, device_id_type=MESH)
    mask_own.start()
    mask_pair.start()
    for cp in qlocals:
        cp.start()
    pl.semaphore_wait(barrier, len(friends))

    def z_copy(k, t):
        src = k_hbm if t == 0 else v_hbm
        zt = z_of(k)
        return remote(src.at[:, cols((zt % 2) * 128, 128)], buf.at[c, b, z, t, a],
                      zs.at[k, t], zr.at[k, t], dev(x, zt, y, c, h))

    def q_copy(i):
        return remote(q_hbm.at[:, cols((1 - g) * 512 + i * 128, 128)], qs.at[1, i],
                      qss.at[i], qsr.at[i], pair)

    def a_copy(k, way):
        zt = z_of(k)
        if way == 0:
            ref, to = buf.at[c, b, zt, :, a], a_dev(1)
        elif way == 1:
            ref, to = buf.at[c, b, zt, :, a], a_dev(-1)
        elif way == 2:
            ref, to = buf.at[c, b, zt, 0, (a + 3) % 4], a_dev(1)
        else:
            ref, to = buf.at[c, b, zt, 1, (a + 1) % 4], a_dev(-1)
        return remote(ref, ref, a_s.at[k, way], a_r.at[k, way], to)

    def b_copy(k, way):
        zt = z_of(k)
        if way == 0:
            ref, to = buf.at[c, b, zt], b_dev(1)
        elif way == 1:
            ref, to = buf.at[c, b, zt], b_dev(-1)
        elif way == 2:
            ref, to = buf.at[c, (b + 3) % 4, zt, 0], b_dev(1)
        else:
            ref, to = buf.at[c, (b + 1) % 4, zt, 1], b_dev(-1)
        return remote(ref, ref, b_s.at[k, way], b_r.at[k, way], to)

    def unit_of(base, i):
        return (base + (4 - i) * (i % 2) * (1 - i // 2) + (i // 2) * (1 + i % 2)) % 4

    def d_copy(k, i):
        ref = buf.at[c, unit_of(b, i), z_of(k)]
        return remote(ref, ref, d_s.at[k, i], d_r.at[k, i], mate)

    for k in (1, 2, 3):
        for t in range(2):
            z_copy(k, t).start()
    for i in range(4):
        q_copy(i).start()
    for cp in locals_:
        cp.wait()
    a_copy(0, 0).start()
    a_copy(0, 1).start()
    wcopy = pltpu.make_async_copy(w_hbm, w, wsem)
    wcopy.start()

    mask_own.wait()
    mask_pair.wait()
    for r, row_chip in ((0, chip), (1, pair_chip)):
        at = (row_chip % 2) * 2 + c
        all8 = mask8[r]
        two = jnp.where(at < 2, jnp.where(at == 0, all8[0:2], all8[2:4]),
                        jnp.where(at == 2, all8[4:6], all8[6:8]))
        open2 = jnp.where(two > 0, 0.0, OFF).astype(jnp.float32)
        wide = jnp.concatenate([jnp.broadcast_to(open2[i:i + 1], (64, 256)) for i in range(2)], axis=0)
        bias[r] = jnp.transpose(wide).reshape(256, 1, 128)
        for i in range(2):
            own_tile = (row_chip * 2 + c) * 2 + i
            dbias[r, i] = bias[r, own_tile]
            bias[r, own_tile] = jnp.full((1, 128), OFF, jnp.float32)

    mx[...] = jnp.full(mx.shape, FLOOR, jnp.float32)
    ls[...] = jnp.zeros(ls.shape, jnp.float32)
    acc[...] = jnp.zeros(acc.shape, jnp.float32)

    def masked(scores, r, rows):
        tiles = [jnp.broadcast_to(jnp.concatenate([row] * 4, axis=1), (64, 512)) for row in rows]
        return scores + jnp.concatenate(tiles, axis=0)

    def dot_keys(keys, r):
        return lax.dot_general(keys, qs[r].reshape(512, HD), (((1,), (1,)), ((), ())),
                               preferred_element_type=jnp.float32)

    def soften(r, scores, best):
        old = mx[r]
        new = jnp.maximum(old, best)
        probs = jnp.exp2((scores - new) * EXP_SCALE)
        shrink = jnp.exp2((old - new) * EXP_SCALE)
        ls[r] = ls[r] * shrink + jnp.sum(probs, axis=0, keepdims=True)
        mx[r] = new
        return probs.astype(jnp.bfloat16), shrink

    def blend(r, probs, shrink, vals):
        acc[r] = acc[r] * shrink + lax.dot_general(
            vals, probs, (((0,), (0,)), ((), ())), preferred_element_type=jnp.float32)

    def first_chip(st, bb, zz):
        return (1 - st) * (bb * 16 + zz * 4) + st * (zz * 4 + bb)

    def score_job(job):
        st, bb, zz, r = job
        rows = []
        for i in range(4):
            tile = (((1 - st) * (bb * 16 + zz * 4 + i) + st * (i * 16 + zz * 4 + bb)) * 2 + st) * 2
            rows += [bias[r, tile], bias[r, tile + 1]]
        scores = masked(dot_keys(buf[st, bb, zz, 0].reshape(512, HD), r), r, rows)
        sbuf[...] = scores
        return jnp.max(scores, axis=0, keepdims=True)

    def run(ks, units, streams):
        count = len(ks) * len(units) * len(streams) * 2

        def pick(values, at):
            out = values[0]
            for i in range(1, len(values)):
                out = jnp.where(at == i, values[i], out)
            return out

        def job_at(n):
            r = n % 2
            other = pick(streams, (n // 2) % len(streams))
            i = pick(units, (n // 2 // len(streams)) % len(units))
            k = pick(ks, n // 2 // len(streams) // len(units))
            st = c * (1 - other) + (1 - c) * other
            return st, unit_of(b * (1 - other) + a * other, i), z_of(k), r

        ends, total = [], 0
        for n in range(count):
            st, bb, zz, r = job_at(n)
            row_chip = chip * (1 - r) + pair_chip * r
            total = total + jnp.where(first_chip(st, bb, zz) <= row_chip, 1, 0)
            ends.append(total)

        def nth(t):
            n = 0
            for end in ends[:-1]:
                n = n + jnp.where(end <= t, 1, 0)
            return job_at(n)

        @pl.when(total > 0)
        def _():
            def body(t, best):
                st, bb, zz, r = nth(t)
                probs, shrink = soften(r, sbuf[...], best)
                following = score_job(nth(jnp.minimum(t + 1, total - 1)))
                blend(r, probs, shrink, buf[st, bb, zz, 1].reshape(512, HD))
                return following

            lax.fori_loop(0, total, body, score_job(nth(0)))

    def diagonal(r, carry):
        zz = z * (1 - r) + pair_z * r
        xx = x * (1 - r) + (3 - x) * r
        aa = y * (1 - c) + xx * c
        bb = xx * (1 - c) + y * c
        scores = masked(dot_keys(buf[c, bb, zz, 0, aa], r), r, [dbias[r, 0], dbias[r, 1]])
        key = lax.broadcasted_iota(jnp.int32, (128, 512), 0)
        row = lax.broadcasted_iota(jnp.int32, (128, 512), 1) % 128
        scores = jnp.where(key <= row, scores, OFF)
        probs, shrink = soften(r, scores, jnp.max(scores, axis=0, keepdims=True))
        blend(r, probs, shrink, buf[c, bb, zz, 1, aa])
        return carry

    def a_forward(k):
        a_copy(k, 0).wait_recv()
        a_copy(k, 2).start()
        a_copy(k, 1).wait_recv()
        a_copy(k, 3).start()

    def a_begin(k):
        z_copy(k, 0).wait_recv()
        z_copy(k, 1).wait_recv()
        a_copy(k, 0).start()
        a_copy(k, 1).start()

    def b_begin(k):
        a_copy(k, 2).wait_recv()
        a_copy(k, 3).wait_recv()
        b_copy(k, 0).start()
        b_copy(k, 1).start()
        d_copy(k, 0).start()

    def d_arrived(*pairs):
        for k, i in pairs:
            d_copy(k, i).wait_recv()

    def near(k):
        b_copy(k, 0).wait_recv()
        b_copy(k, 2).start()
        b_copy(k, 1).wait_recv()
        b_copy(k, 3).start()
        d_copy(k, 1).start()
        d_copy(k, 2).start()

    def far(k):
        b_copy(k, 2).wait_recv()
        b_copy(k, 3).wait_recv()
        d_copy(k, 3).start()

    a_forward(0)
    a_begin(1)
    b_begin(0)
    a_forward(1)
    a_begin(2)
    b_begin(1)
    a_forward(2)
    a_begin(3)
    b_begin(2)
    for cp in qlocals:
        cp.wait()
    for i in range(4):
        q_copy(i).wait()
    a_forward(3)
    b_begin(3)
    run((0, 1, 2), (0,), (0,))
    d_arrived((0, 0), (1, 0), (2, 0), (3, 0))
    near(0)
    run((0, 1, 2), (0,), (1,))
    near(1)
    run((3,), (0,), (0, 1))
    near(2)
    d_arrived((0, 1), (0, 2), (1, 1), (1, 2))
    run((0, 1), (1, 2), (0, 1))
    near(3)
    far(0)
    d_arrived((2, 1), (2, 2))
    run((2,), (1, 2), (0, 1))
    far(1)
    d_arrived((3, 1), (3, 2), (0, 3))
    run((3,), (1, 2), (0, 1))
    lax.fori_loop(0, 2, diagonal, 0)
    far(2)
    d_arrived((1, 3))
    run((0, 1), (3,), (0, 1))
    far(3)
    run((2, 3), (3,), (0,))
    d_arrived((2, 3), (3, 3))
    run((2, 3), (3,), (1,))

    def result(r):
        done = acc[r] / ls[r]
        return [jnp.transpose(done[:, i * 128:(i + 1) * 128]).astype(jnp.bfloat16) for i in range(4)]

    for i, part in enumerate(result(1)):
        osend[:, i * 128:(i + 1) * 128] = part
    o_copy = remote(osend, att.at[g], o_s, o_r, pair)
    o_copy.start()
    for i, part in enumerate(result(0)):
        att[g, :, i * 128:(i + 1) * 128] = part
    wcopy.wait()
    o_copy.wait()

    def p_copy(n):
        return remote(psend.at[n], precv.at[n], p_s.at[n], p_r.at[n], across)

    def project(n, carry):
        at = cols(n * COLS, COLS)
        part = jnp.dot(att[0], w[0:512, at], preferred_element_type=jnp.float32)
        part = part + jnp.dot(att[1], w[512:1024, at], preferred_element_type=jnp.float32)
        upper, lower = part[0:64], part[64:128]
        mine = jnp.where(h == 0, upper, lower)
        theirs = jnp.where(h == 0, lower, upper)
        psend[n] = theirs.astype(jnp.bfloat16)
        p_copy(n).start()
        pown[n] = mine
        return carry

    lax.fori_loop(0, 4096 // COLS, project, 0)

    def finish(n, carry):
        p_copy(n).wait()
        out_ref[:, cols(n * COLS, COLS)] = (pown[n] + precv[n].astype(jnp.float32)).astype(jnp.bfloat16)
        return carry

    lax.fori_loop(0, 4096 // COLS, finish, 0)

    def drain(k, carry):
        for way in range(4):
            a_copy(k, way).wait_send()
            b_copy(k, way).wait_send()
        for i in range(4):
            d_copy(k, i).wait_send()
        return carry

    lax.fori_loop(0, 4, drain, 0)
    for k in (1, 2, 3):
        for t in range(2):
            z_copy(k, t).wait_send()


def per_device(queries, keys, values, tile_mask, out_weight):
    dma = pltpu.SemaphoreType.DMA
    bf, f32 = jnp.bfloat16, jnp.float32
    n = 4096 // COLS
    return pl.pallas_call(
        kernel,
        out_shape=jax.ShapeDtypeStruct((64, 4096), bf),
        in_specs=[pl.BlockSpec(memory_space=pltpu.HBM)] * 5,
        out_specs=pl.BlockSpec(memory_space=pltpu.VMEM),
        scratch_shapes=[
            pltpu.VMEM((2, 4, 4, 2, 4, 128, 128), bf),
            pltpu.VMEM((2, 4, 128, 128), bf),
            pltpu.VMEM((1024, 4096), bf),
            pltpu.VMEM((2, 8, 256), jnp.int32),
            pltpu.VMEM((2, 256, 1, 128), f32),
            pltpu.VMEM((2, 2, 1, 128), f32),
            pltpu.VMEM((2, 1, 512), f32),
            pltpu.VMEM((2, 1, 512), f32),
            pltpu.VMEM((2, 128, 512), f32),
            pltpu.VMEM((512, 512), f32),
            pltpu.VMEM((2, 128, 512), bf),
            pltpu.VMEM((128, 512), bf),
            pltpu.VMEM((n, 64, COLS), f32),
            pltpu.VMEM((n, 64, COLS), bf),
            pltpu.VMEM((n, 64, COLS), bf),
            dma((2,)), dma((4,)), dma, dma((2,)),
            dma((4, 2)), dma((4, 2)), dma((4,)), dma((4,)),
            dma((4, 4)), dma((4, 4)), dma((4, 4)), dma((4, 4)), dma((4, 4)), dma((4, 4)),
            dma, dma, dma((n,)), dma((n,)),
        ],
        compiler_params=pltpu.CompilerParams(
            collective_id=0, has_side_effects=True, vmem_limit_bytes=48 * 1024 * 1024),
    )(queries, keys, values, tile_mask, out_weight)


def solution(mesh):
    placed = (P("seq", "head"), P("seq", "head"), P("seq", "head"), P(), P("head", None))
    return jax.shard_map(
        per_device, mesh=mesh, in_specs=placed, out_specs=P(("seq", "head"), None), check_vma=False
    )
```

```python
import math

import jax
import jax.numpy as jnp
from jax import lax
from jax.experimental import pallas as pl
from jax.experimental.pallas import tpu as pltpu
from jax.sharding import PartitionSpec as P

HD = 128
MESH = pl.DeviceIdType.MESH
OFF = -1e30
FLOOR = -1e6
EXP_SCALE = math.log2(math.e) / math.sqrt(HD)
COLS = 512


def kernel(q_hbm, k_hbm, v_hbm, mask_hbm, w_hbm, out_ref,
           buf, kv, qs, w, mask8, bias, dbias, mx, ls, acc, sbuf, att, osend, pown, psend, precv,
           lsem, qlsem, wsem, msem, zs, zr, qss, qsr, a_s, a_r, b_s, b_r, d_s, d_r, o_s, o_r, p_s, p_r):
    s = lax.axis_index("seq")
    h = lax.axis_index("head")
    c = s % 2
    y = (s // 2) % 4
    z = (s // 8) % 4
    x = s // 32
    a = y * (1 - c) + x * c
    b = x * (1 - c) + y * c
    g = z % 2
    chip = x * 16 + z * 4 + y
    pair_z = z + 1 - 2 * g
    pair_chip = (3 - x) * 16 + pair_z * 4 + y

    def dev(xx, zz, yy, cc, hh):
        return {"seq": ((xx * 4 + zz) * 4 + yy) * 2 + cc, "head": hh}

    def a_dev(d):
        return dev((x + c * d + 4) % 4, z, (y + (1 - c) * d + 4) % 4, c, h)

    def b_dev(d):
        return dev((x + (1 - c) * d + 4) % 4, z, (y + c * d + 4) % 4, c, h)

    def z_of(k):
        return ((z // 2 + k // 2) % 2) * 2 + (z % 2 + k % 2) % 2

    mate = dev(x, z, y, 1 - c, h)
    pair = dev(3 - x, pair_z, y, c, h)
    across = dev(x, z, y, c, 1 - h)

    def remote(src, dst, ss, rs, to):
        return pltpu.make_async_remote_copy(
            src_ref=src, dst_ref=dst, send_sem=ss, recv_sem=rs, device_id=to, device_id_type=MESH)

    def cols(start, size):
        return pl.ds(pl.multiple_of(start, 128), size)

    locals_ = [
        pltpu.make_async_copy(k_hbm.at[:, cols(g * 128, 128)], buf.at[c, b, z, 0, a], lsem.at[0]),
        pltpu.make_async_copy(v_hbm.at[:, cols(g * 128, 128)], buf.at[c, b, z, 1, a], lsem.at[1]),
    ]
    qlocals = [
        pltpu.make_async_copy(q_hbm.at[:, cols(g * 512 + i * 128, 128)], qs.at[0, i], qlsem.at[i])
        for i in range(4)
    ]
    mask_own = pltpu.make_async_copy(
        mask_hbm.at[pl.ds(pl.multiple_of((chip // 2) * 8, 8), 8)], mask8.at[0], msem.at[0])
    mask_pair = pltpu.make_async_copy(
        mask_hbm.at[pl.ds(pl.multiple_of((pair_chip // 2) * 8, 8), 8)], mask8.at[1], msem.at[1])
    stage = [pltpu.make_async_copy(k_hbm, kv.at[0], lsem.at[2]), pltpu.make_async_copy(v_hbm, kv.at[1], lsem.at[3])]
    for cp in stage + locals_:
        cp.start()

    barrier = pltpu.get_barrier_semaphore()
    friends = [a_dev(1), a_dev(-1), a_dev(2), b_dev(1), b_dev(-1), mate, pair, across] + [
        dev(x, z_of(k), y, c, h) for k in (1, 2, 3)]
    for f in friends:
        pl.semaphore_signal(barrier, inc=1, device_id=f, device_id_type=MESH)
    mask_own.start()
    mask_pair.start()
    for cp in qlocals:
        cp.start()
    pl.semaphore_wait(barrier, len(friends))

    def z_copy(k, t):
        zt = z_of(k)
        return remote(kv.at[t, :, cols((zt % 2) * 128, 128)], buf.at[c, b, z, t, a],
                      zs.at[k, t], zr.at[k, t], dev(x, zt, y, c, h))

    def q_copy(i):
        return remote(q_hbm.at[:, cols((1 - g) * 512 + i * 128, 128)], qs.at[1, i],
                      qss.at[i], qsr.at[i], pair)

    def a_copy(k, way):
        zt = z_of(k)
        if way == 0:
            ref, to = buf.at[c, b, zt, :, a], a_dev(1)
        elif way == 1:
            ref, to = buf.at[c, b, zt, :, a], a_dev(-1)
        else:
            ref, to = buf.at[c, b, zt, :, a], a_dev(2)
        return remote(ref, ref, a_s.at[k, way], a_r.at[k, way], to)

    def b_copy(k, way):
        zt = z_of(k)
        if way == 0:
            ref, to = buf.at[c, b, zt], b_dev(1)
        elif way == 1:
            ref, to = buf.at[c, b, zt], b_dev(-1)
        elif way == 2:
            ref, to = buf.at[c, (b + 3) % 4, zt, 0], b_dev(1)
        else:
            ref, to = buf.at[c, (b + 1) % 4, zt, 1], b_dev(-1)
        return remote(ref, ref, b_s.at[k, way], b_r.at[k, way], to)

    def unit_of(base, i):
        return (base + (4 - i) * (i % 2) * (1 - i // 2) + (i // 2) * (1 + i % 2)) % 4

    def d_copy(k, i):
        ref = buf.at[c, unit_of(b, i), z_of(k)]
        return remote(ref, ref, d_s.at[k, i], d_r.at[k, i], mate)

    for cp in stage:
        cp.wait()
    for k in (1, 2, 3):
        for t in range(2):
            z_copy(k, t).start()
    for i in range(4):
        q_copy(i).start()
    for cp in locals_:
        cp.wait()
    for way in range(3):
        a_copy(0, way).start()
    wcopy = pltpu.make_async_copy(w_hbm, w, wsem)
    wcopy.start()

    mask_own.wait()
    mask_pair.wait()
    for r, row_chip in ((0, chip), (1, pair_chip)):
        at = (row_chip % 2) * 2 + c
        all8 = mask8[r]
        two = jnp.where(at < 2, jnp.where(at == 0, all8[0:2], all8[2:4]),
                        jnp.where(at == 2, all8[4:6], all8[6:8]))
        open2 = jnp.where(two > 0, 0.0, OFF).astype(jnp.float32)
        wide = jnp.concatenate([jnp.broadcast_to(open2[i:i + 1], (64, 256)) for i in range(2)], axis=0)
        bias[r] = jnp.transpose(wide).reshape(256, 1, 128)
        for i in range(2):
            own_tile = (row_chip * 2 + c) * 2 + i
            dbias[r, i] = bias[r, own_tile]
            bias[r, own_tile] = jnp.full((1, 128), OFF, jnp.float32)

    mx[...] = jnp.full(mx.shape, FLOOR, jnp.float32)
    ls[...] = jnp.zeros(ls.shape, jnp.float32)
    acc[...] = jnp.zeros(acc.shape, jnp.float32)

    def masked(scores, r, rows):
        tiles = [jnp.broadcast_to(jnp.concatenate([row] * 4, axis=1), (64, 512)) for row in rows]
        return scores + jnp.concatenate(tiles, axis=0)

    def dot_keys(keys, r):
        return lax.dot_general(keys, qs[r].reshape(512, HD), (((1,), (1,)), ((), ())),
                               preferred_element_type=jnp.float32)

    def soften(r, scores, best):
        old = mx[r]
        new = jnp.maximum(old, best)
        probs = jnp.exp2((scores - new) * EXP_SCALE)
        shrink = jnp.exp2((old - new) * EXP_SCALE)
        ls[r] = ls[r] * shrink + jnp.sum(probs, axis=0, keepdims=True)
        mx[r] = new
        return probs.astype(jnp.bfloat16), shrink

    def blend(r, probs, shrink, vals):
        acc[r] = acc[r] * shrink + lax.dot_general(
            vals, probs, (((0,), (0,)), ((), ())), preferred_element_type=jnp.float32)

    def first_chip(st, bb, zz):
        return (1 - st) * (bb * 16 + zz * 4) + st * (zz * 4 + bb)

    def score_job(job):
        st, halves, r = job[0], ((job[1], job[2], 0), (job[3], job[4], job[5])), job[6]
        rows, keys = [], []
        for bb, zz, first in halves:
            keys.append(buf[st, bb, zz, 0, pl.ds(first, 2)].reshape(256, HD))
            for i in range(2):
                tile = (((1 - st) * (bb * 16 + zz * 4 + first + i)
                         + st * ((first + i) * 16 + zz * 4 + bb)) * 2 + st) * 2
                rows += [bias[r, tile], bias[r, tile + 1]]
        scores = masked(dot_keys(jnp.concatenate(keys, axis=0), r), r, rows)
        sbuf[...] = scores
        return jnp.max(scores, axis=0, keepdims=True)

    def weigh_job(job):
        return soften(job[6], sbuf[...], job[7])

    def blend_job(job, probs, shrink):
        st = job[0]
        vals = [buf[st, job[1], job[2], 1, 0:2].reshape(256, HD),
                buf[st, job[3], job[4], 1, pl.ds(job[5], 2)].reshape(256, HD)]
        blend(job[6], probs, shrink, jnp.concatenate(vals, axis=0))

    def flush(job):
        probs, shrink = weigh_job(job)
        blend_job(job, probs, shrink)

    def pick(values, at):
        out = values[0]
        for i in range(1, len(values)):
            out = jnp.where(at == i, values[i], out)
        return out

    def run(units, streams, rows, pending=None):
        count = len(units) * len(streams) * len(rows)

        def parts(n):
            u = n % len(units)
            r = pick(rows, (n // len(units)) % len(rows))
            other = pick(streams, n // len(units) // len(rows))
            st = c * (1 - other) + (1 - c) * other
            early = 1 - (x * (1 - r) + (3 - x) * r) // 2
            base = b * (1 - other) + a * other

            def place(v):
                return unit_of(base, pick([i for _, i in units], v)), z_of(pick([k for k, _ in units], v))

            here = place(u)
            there = place(u - u % 2 + 1)
            return st, u % 2, here, there, r, st * early

        def job_at(n):
            st, _, here, there, r, joined = parts(n)
            return (st, here[0], here[1], here[0] * (1 - joined) + there[0] * joined,
                    here[1] * (1 - joined) + there[1] * joined, 2 * (1 - joined), r)

        ends, total = [], 0
        for n in range(count):
            st, odd, here, there, r, joined = parts(n)
            row_chip = chip * (1 - r) + pair_chip * r
            mine = jnp.where(first_chip(st, *here) <= row_chip, 1, 0)
            other_one = jnp.where(first_chip(st, *there) <= row_chip, 1, 0)
            use = mine * (1 - joined) + joined * (1 - odd) * jnp.maximum(mine, other_one)
            total = total + use
            ends.append(total)

        def nth(t):
            n = 0
            for end in ends[:-1]:
                n = n + jnp.where(end <= t, 1, 0)
            return tuple(jnp.asarray(v, jnp.int32) for v in job_at(n))

        def body(t, job):
            probs, shrink = weigh_job(job)
            following = nth(t)
            best = score_job(following)
            blend_job(job, probs, shrink)
            return following + (best,)

        if pending is not None:
            return lax.fori_loop(0, total, body, pending)
        start = nth(0)
        return lax.fori_loop(1, total, body, start + (score_job(start),))

    def diagonal(r, carry):
        zz = z * (1 - r) + pair_z * r
        xx = x * (1 - r) + (3 - x) * r
        aa = y * (1 - c) + xx * c
        bb = xx * (1 - c) + y * c
        scores = masked(dot_keys(buf[c, bb, zz, 0, aa], r), r, [dbias[r, 0], dbias[r, 1]])
        key = lax.broadcasted_iota(jnp.int32, (128, 512), 0)
        row = lax.broadcasted_iota(jnp.int32, (128, 512), 1) % 128
        scores = jnp.where(key <= row, scores, OFF)
        probs, shrink = soften(r, scores, jnp.max(scores, axis=0, keepdims=True))
        blend(r, probs, shrink, buf[c, bb, zz, 1, aa])
        return carry

    def a_begin(k):
        z_copy(k, 0).wait_recv()
        z_copy(k, 1).wait_recv()
        for way in range(3):
            a_copy(k, way).start()

    def b_begin(k):
        for way in range(3):
            a_copy(k, way).wait_recv()
        b_copy(k, 0).start()
        b_copy(k, 1).start()
        d_copy(k, 0).start()

    def d_arrived(*pairs):
        for k, i in pairs:
            d_copy(k, i).wait_recv()

    def near(k):
        b_copy(k, 0).wait_recv()
        b_copy(k, 2).start()
        b_copy(k, 1).wait_recv()
        b_copy(k, 3).start()
        d_copy(k, 1).start()
        d_copy(k, 2).start()

    def far(k):
        b_copy(k, 2).wait_recv()
        b_copy(k, 3).wait_recv()
        d_copy(k, 3).start()

    def own(*ks):
        return tuple((k, 0) for k in ks)

    def side(k):
        return ((k, 1), (k, 2))

    def opposite(*ks):
        return tuple((k, 3) for k in ks)

    a_begin(1)
    b_begin(0)
    a_begin(2)
    a_begin(3)
    for cp in qlocals:
        cp.wait()
    for i in range(4):
        q_copy(i).wait()
    b_begin(1)
    job = run(own(0, 1), (0,), (0, 1))
    b_begin(2)
    b_begin(3)
    d_arrived((0, 0), (1, 0))
    job = run(own(0, 1), (1,), (0, 1), job)
    near(0)
    job = run(own(2, 3), (0,), (0, 1), job)
    near(1)
    d_arrived((2, 0), (3, 0))
    job = run(own(2, 3), (1,), (0, 1), job)
    near(2)
    d_arrived((0, 1), (0, 2))
    job = run(side(0), (0, 1), (1,), job)
    near(3)
    lax.fori_loop(0, 2, diagonal, 0)
    d_arrived((1, 1), (1, 2))
    job = run(side(1), (0, 1), (1,), job)
    job = run(side(0), (0, 1), (0,), job)
    far(0)
    d_arrived((2, 1), (2, 2))
    job = run(side(2), (0, 1), (1,), job)
    far(1)
    d_arrived((3, 1), (3, 2))
    job = run(side(3), (0, 1), (1,), job)
    job = run(side(1), (0, 1), (0,), job)
    far(2)
    d_arrived((0, 3), (1, 3))
    job = run(opposite(0, 1), (0, 1), (1,), job)
    far(3)
    job = run(opposite(2, 3), (0,), (1,), job)
    d_arrived((2, 3), (3, 3))
    job = run(opposite(2, 3), (1,), (1,), job)
    flush(job)

    def result(r):
        done = acc[r] / ls[r]
        return [jnp.transpose(done[:, i * 128:(i + 1) * 128]).astype(jnp.bfloat16) for i in range(4)]

    for i, part in enumerate(result(1)):
        osend[:, i * 128:(i + 1) * 128] = part
    o_copy = remote(osend, att.at[g], o_s, o_r, pair)
    o_copy.start()
    rest = side(2) + side(3) + opposite(0, 1, 2, 3)
    flush(run(rest, (0, 1), (0,)))
    for i, part in enumerate(result(0)):
        att[g, :, i * 128:(i + 1) * 128] = part
    wcopy.wait()
    o_copy.wait()

    def p_copy(n):
        return remote(psend.at[n], precv.at[n], p_s.at[n], p_r.at[n], across)

    def project(n, carry):
        at = cols(n * COLS, COLS)
        part = jnp.dot(att[0], w[0:512, at], preferred_element_type=jnp.float32)
        part = part + jnp.dot(att[1], w[512:1024, at], preferred_element_type=jnp.float32)
        upper, lower = part[0:64], part[64:128]
        mine = jnp.where(h == 0, upper, lower)
        theirs = jnp.where(h == 0, lower, upper)
        psend[n] = theirs.astype(jnp.bfloat16)
        p_copy(n).start()
        pown[n] = mine
        return carry

    lax.fori_loop(0, 4096 // COLS, project, 0)

    def finish(n, carry):
        p_copy(n).wait()
        out_ref[:, cols(n * COLS, COLS)] = (pown[n] + precv[n].astype(jnp.float32)).astype(jnp.bfloat16)
        return carry

    lax.fori_loop(0, 4096 // COLS, finish, 0)

    def drain(k, carry):
        for way in range(3):
            a_copy(k, way).wait_send()
        for way in range(4):
            b_copy(k, way).wait_send()
        for i in range(4):
            d_copy(k, i).wait_send()
        return carry

    lax.fori_loop(0, 4, drain, 0)
    for k in (1, 2, 3):
        for t in range(2):
            z_copy(k, t).wait_send()


def per_device(queries, keys, values, tile_mask, out_weight):
    dma = pltpu.SemaphoreType.DMA
    bf, f32 = jnp.bfloat16, jnp.float32
    n = 4096 // COLS
    return pl.pallas_call(
        kernel,
        out_shape=jax.ShapeDtypeStruct((64, 4096), bf),
        in_specs=[pl.BlockSpec(memory_space=pltpu.HBM)] * 5,
        out_specs=pl.BlockSpec(memory_space=pltpu.VMEM),
        scratch_shapes=[
            pltpu.VMEM((2, 4, 4, 2, 4, 128, 128), bf),
            pltpu.VMEM((2, 128, 256), bf),
            pltpu.VMEM((2, 4, 128, 128), bf),
            pltpu.VMEM((1024, 4096), bf),
            pltpu.VMEM((2, 8, 256), jnp.int32),
            pltpu.VMEM((2, 256, 1, 128), f32),
            pltpu.VMEM((2, 2, 1, 128), f32),
            pltpu.VMEM((2, 1, 512), f32),
            pltpu.VMEM((2, 1, 512), f32),
            pltpu.VMEM((2, 128, 512), f32),
            pltpu.VMEM((512, 512), f32),
            pltpu.VMEM((2, 128, 512), bf),
            pltpu.VMEM((128, 512), bf),
            pltpu.VMEM((n, 64, COLS), f32),
            pltpu.VMEM((n, 64, COLS), bf),
            pltpu.VMEM((n, 64, COLS), bf),
            dma((4,)), dma((4,)), dma, dma((2,)),
            dma((4, 2)), dma((4, 2)), dma((4,)), dma((4,)),
            dma((4, 3)), dma((4, 3)), dma((4, 4)), dma((4, 4)), dma((4, 4)), dma((4, 4)),
            dma, dma, dma((n,)), dma((n,)),
        ],
        compiler_params=pltpu.CompilerParams(
            collective_id=0, has_side_effects=True, vmem_limit_bytes=67043328),
    )(queries, keys, values, tile_mask, out_weight)


def solution(mesh):
    placed = (P("seq", "head"), P("seq", "head"), P("seq", "head"), P(), P("head", None))
    return jax.shard_map(
        per_device, mesh=mesh, in_specs=placed, out_specs=P(("seq", "head"), None), check_vma=False
    )
```

```python
import math

import jax
import jax.numpy as jnp
from jax import lax
from jax.experimental import pallas as pl
from jax.experimental.pallas import tpu as pltpu
from jax.sharding import PartitionSpec as P

HD = 128
MESH = pl.DeviceIdType.MESH
OFF = -1e30
FLOOR = -1e6
EXP_SCALE = math.log2(math.e) / math.sqrt(HD)
COLS = 512


def kernel(q_hbm, k_hbm, v_hbm, mask_hbm, w_hbm, out_ref,
           buf, kv, qs, w, wo, mask8, bias, dbias, mx, ls, acc, sbuf, att, attx, osend, tot,
           lsem, qlsem, wsem, msem, zs, zr, qss, qsr, a_s, a_r, b_s, b_r, d_s, d_r, o_s, o_r,
           wf_s, wf_r, wa_s, wa_r, wb_s, wb_r, wg_s, wg_r, wd_s, wd_r, wh_s, wh_r, x_s, x_r):
    s = lax.axis_index("seq")
    h = lax.axis_index("head")
    c = s % 2
    y = (s // 2) % 4
    z = (s // 8) % 4
    x = s // 32
    a = y * (1 - c) + x * c
    b = x * (1 - c) + y * c
    g = z % 2
    chip = x * 16 + z * 4 + y
    pair_z = z + 1 - 2 * g
    pair_chip = (3 - x) * 16 + pair_z * 4 + y

    def dev(xx, zz, yy, cc, hh):
        return {"seq": ((xx * 4 + zz) * 4 + yy) * 2 + cc, "head": hh}

    def a_dev(d):
        return dev((x + c * d + 4) % 4, z, (y + (1 - c) * d + 4) % 4, c, h)

    def b_dev(d):
        return dev((x + (1 - c) * d + 4) % 4, z, (y + c * d + 4) % 4, c, h)

    def z_of(k):
        return ((z // 2 + k // 2) % 2) * 2 + (z % 2 + k % 2) % 2

    mate = dev(x, z, y, 1 - c, h)
    pair = dev(3 - x, pair_z, y, c, h)
    across = dev(x, z, y, c, 1 - h)

    def remote(src, dst, ss, rs, to):
        return pltpu.make_async_remote_copy(
            src_ref=src, dst_ref=dst, send_sem=ss, recv_sem=rs, device_id=to, device_id_type=MESH)

    def cols(start, size):
        return pl.ds(pl.multiple_of(start, 128), size)

    locals_ = [
        pltpu.make_async_copy(k_hbm.at[:, cols(g * 128, 128)], buf.at[c, b, z, 0, a], lsem.at[0]),
        pltpu.make_async_copy(v_hbm.at[:, cols(g * 128, 128)], buf.at[c, b, z, 1, a], lsem.at[1]),
    ]
    qlocals = [
        pltpu.make_async_copy(q_hbm.at[:, cols(g * 512 + i * 128, 128)], qs.at[0, i], qlsem.at[i])
        for i in range(4)
    ]
    mask_own = pltpu.make_async_copy(
        mask_hbm.at[pl.ds(pl.multiple_of((chip // 2) * 8, 8), 8)], mask8.at[0], msem.at[0])
    mask_pair = pltpu.make_async_copy(
        mask_hbm.at[pl.ds(pl.multiple_of((pair_chip // 2) * 8, 8), 8)], mask8.at[1], msem.at[1])
    stage = [pltpu.make_async_copy(k_hbm, kv.at[0], lsem.at[2]), pltpu.make_async_copy(v_hbm, kv.at[1], lsem.at[3])]
    for cp in stage + locals_:
        cp.start()

    barrier = pltpu.get_barrier_semaphore()
    friends = [a_dev(1), a_dev(-1), a_dev(2), b_dev(1), b_dev(-1), mate, pair, across] + [
        dev(x, z_of(k), y, c, h) for k in (1, 2, 3)]
    for f in friends:
        pl.semaphore_signal(barrier, inc=1, device_id=f, device_id_type=MESH)
    mask_own.start()
    mask_pair.start()
    for cp in qlocals:
        cp.start()
    pl.semaphore_wait(barrier, len(friends))

    def z_copy(k, t):
        zt = z_of(k)
        return remote(kv.at[t, :, cols((zt % 2) * 128, 128)], buf.at[c, b, z, t, a],
                      zs.at[k, t], zr.at[k, t], dev(x, zt, y, c, h))

    def q_copy(i):
        return remote(q_hbm.at[:, cols((1 - g) * 512 + i * 128, 128)], qs.at[1, i],
                      qss.at[i], qsr.at[i], pair)

    def a_copy(k, way):
        zt = z_of(k)
        if way == 0:
            ref, to = buf.at[c, b, zt, :, a], a_dev(1)
        elif way == 1:
            ref, to = buf.at[c, b, zt, :, a], a_dev(-1)
        else:
            ref, to = buf.at[c, b, zt, :, a], a_dev(2)
        return remote(ref, ref, a_s.at[k, way], a_r.at[k, way], to)

    def b_copy(k, way):
        zt = z_of(k)
        if way == 0:
            ref, to = buf.at[c, b, zt], b_dev(1)
        elif way == 1:
            ref, to = buf.at[c, b, zt], b_dev(-1)
        elif way == 2:
            ref, to = buf.at[c, (b + 3) % 4, zt, 0], b_dev(1)
        else:
            ref, to = buf.at[c, (b + 1) % 4, zt, 1], b_dev(-1)
        return remote(ref, ref, b_s.at[k, way], b_r.at[k, way], to)

    def unit_of(base, i):
        return (base + (4 - i) * (i % 2) * (1 - i // 2) + (i // 2) * (1 + i % 2)) % 4

    def d_copy(k, i):
        ref = buf.at[c, unit_of(b, i), z_of(k)]
        return remote(ref, ref, d_s.at[k, i], d_r.at[k, i], mate)

    def wf_copy(i):
        slot = (a + 2 * i) % 4
        row = pl.multiple_of(((c * 4 + b) * 4 + slot) * 32, 32)
        return remote(w_hbm.at[pl.ds(row, 32)], wo.at[c, b, slot], wf_s.at[i], wf_r.at[i], across)

    def wa_copy(way):
        ref = wo.at[c, b, a]
        return remote(ref, ref, wa_s.at[way], wa_r.at[way], a_dev(1 - 2 * way))

    def slot_of(j):
        return (a + (0, 3, 1, 2)[j]) % 4

    def wb_copy(way, j):
        ref = wo.at[c, b, slot_of(j)]
        return remote(ref, ref, wb_s.at[way, j], wb_r.at[way, j], b_dev(1 - 2 * way))

    def wg_copy(j):
        ref = wo.at[c, (b + (3, 3, 1, 1)[j]) % 4, slot_of(j)]
        return remote(ref, ref, wg_s.at[j], wg_r.at[j], b_dev((1, 1, -1, -1)[j]))

    def wh_copy(j):
        ref = wo.at[c, (b + 2) % 4, slot_of(j)]
        return remote(ref, ref, wh_s.at[j], wh_r.at[j], mate)

    def w_forward(j):
        wb_copy((0, 0, 1, 1)[j], j).wait_recv()
        wg_copy(j).start()

    def wd_copy(i):
        ref = wo.at[c, unit_of(b, i)]
        return remote(ref, ref, wd_s.at[i], wd_r.at[i], mate)

    for cp in stage:
        cp.wait()
    for k in (1, 2, 3):
        for t in range(2):
            z_copy(k, t).start()
    for i in range(4):
        q_copy(i).start()
    wf_copy(0).start()
    for cp in locals_:
        cp.wait()
    for way in range(3):
        a_copy(0, way).start()
    wcopy = pltpu.make_async_copy(w_hbm, w, wsem)
    wcopy.start()

    mask_own.wait()
    mask_pair.wait()
    for r, row_chip in ((0, chip), (1, pair_chip)):
        at = (row_chip % 2) * 2 + c
        all8 = mask8[r]
        two = jnp.where(at < 2, jnp.where(at == 0, all8[0:2], all8[2:4]),
                        jnp.where(at == 2, all8[4:6], all8[6:8]))
        open2 = jnp.where(two > 0, 0.0, OFF).astype(jnp.float32)
        wide = jnp.concatenate([jnp.broadcast_to(open2[i:i + 1], (64, 256)) for i in range(2)], axis=0)
        bias[r] = jnp.transpose(wide).reshape(256, 1, 128)
        for i in range(2):
            own_tile = (row_chip * 2 + c) * 2 + i
            dbias[r, i] = bias[r, own_tile]
            bias[r, own_tile] = jnp.full((1, 128), OFF, jnp.float32)

    mx[...] = jnp.full(mx.shape, FLOOR, jnp.float32)
    ls[...] = jnp.zeros(ls.shape, jnp.float32)
    acc[...] = jnp.zeros(acc.shape, jnp.float32)

    def masked(scores, r, rows):
        tiles = [jnp.broadcast_to(jnp.concatenate([row] * 4, axis=1), (64, 512)) for row in rows]
        return scores + jnp.concatenate(tiles, axis=0)

    def dot_keys(keys, r):
        return lax.dot_general(keys, qs[r].reshape(512, HD), (((1,), (1,)), ((), ())),
                               preferred_element_type=jnp.float32)

    def soften(r, scores, best):
        old = mx[r]
        new = jnp.maximum(old, best)
        probs = jnp.exp2((scores - new) * EXP_SCALE)
        shrink = jnp.exp2((old - new) * EXP_SCALE)
        ls[r] = ls[r] * shrink + jnp.sum(probs, axis=0, keepdims=True)
        mx[r] = new
        return probs.astype(jnp.bfloat16), shrink

    def blend(r, probs, shrink, vals):
        acc[r] = acc[r] * shrink + lax.dot_general(
            vals, probs, (((0,), (0,)), ((), ())), preferred_element_type=jnp.float32)

    def first_chip(st, bb, zz):
        return (1 - st) * (bb * 16 + zz * 4) + st * (zz * 4 + bb)

    def score_job(job):
        st, halves, r = job[0], ((job[1], job[2], 0), (job[3], job[4], job[5])), job[6]
        rows, keys = [], []
        for bb, zz, first in halves:
            keys.append(buf[st, bb, zz, 0, pl.ds(first, 2)].reshape(256, HD))
            for i in range(2):
                tile = (((1 - st) * (bb * 16 + zz * 4 + first + i)
                         + st * ((first + i) * 16 + zz * 4 + bb)) * 2 + st) * 2
                rows += [bias[r, tile], bias[r, tile + 1]]
        scores = masked(dot_keys(jnp.concatenate(keys, axis=0), r), r, rows)
        sbuf[...] = scores
        return jnp.max(scores, axis=0, keepdims=True)

    def weigh_job(job):
        return soften(job[6], sbuf[...], job[7])

    def blend_job(job, probs, shrink):
        st = job[0]
        vals = [buf[st, job[1], job[2], 1, 0:2].reshape(256, HD),
                buf[st, job[3], job[4], 1, pl.ds(job[5], 2)].reshape(256, HD)]
        blend(job[6], probs, shrink, jnp.concatenate(vals, axis=0))

    def flush(job):
        probs, shrink = weigh_job(job)
        blend_job(job, probs, shrink)

    def pick(values, at):
        out = values[0]
        for i in range(1, len(values)):
            out = jnp.where(at == i, values[i], out)
        return out

    def run(units, streams, rows, pending=None):
        count = len(units) * len(streams) * len(rows)

        def parts(n):
            u = n % len(units)
            r = pick(rows, (n // len(units)) % len(rows))
            other = pick(streams, n // len(units) // len(rows))
            st = c * (1 - other) + (1 - c) * other
            early = 1 - (x * (1 - r) + (3 - x) * r) // 2
            base = b * (1 - other) + a * other

            def place(v):
                return unit_of(base, pick([i for _, i in units], v)), z_of(pick([k for k, _ in units], v))

            here = place(u)
            there = place(u - u % 2 + 1)
            return st, u % 2, here, there, r, st * early

        def job_at(n):
            st, _, here, there, r, joined = parts(n)
            return (st, here[0], here[1], here[0] * (1 - joined) + there[0] * joined,
                    here[1] * (1 - joined) + there[1] * joined, 2 * (1 - joined), r)

        ends, total = [], 0
        for n in range(count):
            st, odd, here, there, r, joined = parts(n)
            row_chip = chip * (1 - r) + pair_chip * r
            mine = jnp.where(first_chip(st, *here) <= row_chip, 1, 0)
            other_one = jnp.where(first_chip(st, *there) <= row_chip, 1, 0)
            use = mine * (1 - joined) + joined * (1 - odd) * jnp.maximum(mine, other_one)
            total = total + use
            ends.append(total)

        def nth(t):
            n = 0
            for end in ends[:-1]:
                n = n + jnp.where(end <= t, 1, 0)
            return tuple(jnp.asarray(v, jnp.int32) for v in job_at(n))

        def body(t, job):
            probs, shrink = weigh_job(job)
            following = nth(t)
            best = score_job(following)
            blend_job(job, probs, shrink)
            return following + (best,)

        if pending is not None:
            return lax.fori_loop(0, total, body, pending)
        start = nth(0)
        return lax.fori_loop(1, total, body, start + (score_job(start),))

    def diagonal(r, carry):
        zz = z * (1 - r) + pair_z * r
        xx = x * (1 - r) + (3 - x) * r
        aa = y * (1 - c) + xx * c
        bb = xx * (1 - c) + y * c
        scores = masked(dot_keys(buf[c, bb, zz, 0, aa], r), r, [dbias[r, 0], dbias[r, 1]])
        key = lax.broadcasted_iota(jnp.int32, (128, 512), 0)
        row = lax.broadcasted_iota(jnp.int32, (128, 512), 1) % 128
        scores = jnp.where(key <= row, scores, OFF)
        probs, shrink = soften(r, scores, jnp.max(scores, axis=0, keepdims=True))
        blend(r, probs, shrink, buf[c, bb, zz, 1, aa])
        return carry

    def a_begin(k):
        z_copy(k, 0).wait_recv()
        z_copy(k, 1).wait_recv()
        for way in range(3):
            a_copy(k, way).start()

    def b_begin(k):
        for way in range(3):
            a_copy(k, way).wait_recv()
        b_copy(k, 0).start()
        b_copy(k, 1).start()
        d_copy(k, 0).start()

    def d_arrived(*pairs):
        for k, i in pairs:
            d_copy(k, i).wait_recv()

    def near(k):
        b_copy(k, 0).wait_recv()
        b_copy(k, 2).start()
        b_copy(k, 1).wait_recv()
        b_copy(k, 3).start()
        d_copy(k, 1).start()
        d_copy(k, 2).start()

    def far(k):
        b_copy(k, 2).wait_recv()
        b_copy(k, 3).wait_recv()
        d_copy(k, 3).start()

    def own(*ks):
        return tuple((k, 0) for k in ks)

    def side(k):
        return ((k, 1), (k, 2))

    def opposite(*ks):
        return tuple((k, 3) for k in ks)

    a_begin(1)
    b_begin(0)
    a_begin(2)
    a_begin(3)
    for cp in qlocals:
        cp.wait()
    for i in range(4):
        q_copy(i).wait()
    b_begin(1)
    job = run(own(0, 1), (0,), (0, 1))
    b_begin(2)
    b_begin(3)
    d_arrived((0, 0), (1, 0))
    job = run(own(0, 1), (1,), (0, 1), job)
    near(0)
    wf_copy(1).start()
    job = run(own(2, 3), (0,), (0, 1), job)
    near(1)
    d_arrived((2, 0), (3, 0))
    job = run(own(2, 3), (1,), (0, 1), job)
    near(2)
    d_arrived((0, 1), (0, 2))
    job = run(side(0), (0, 1), (1,), job)
    near(3)
    wf_copy(0).wait_recv()
    for way in range(2):
        wa_copy(way).start()
        wb_copy(way, 0).start()
    lax.fori_loop(0, 2, diagonal, 0)
    d_arrived((1, 1), (1, 2))
    job = run(side(1), (0, 1), (1,), job)
    job = run(side(0), (0, 1), (0,), job)
    far(0)
    d_arrived((2, 1), (2, 2))
    job = run(side(2), (0, 1), (1,), job)
    far(1)
    d_arrived((3, 1), (3, 2))
    job = run(side(3), (0, 1), (1,), job)
    job = run(side(1), (0, 1), (0,), job)
    far(2)
    for way in range(2):
        wa_copy(way).wait_recv()
    for j in (1, 2):
        for way in range(2):
            wb_copy(way, j).start()
    d_arrived((0, 3), (1, 3))
    job = run(opposite(0, 1), (0, 1), (1,), job)
    job = run(side(2), (0, 1), (0,), job)
    far(3)
    wf_copy(1).wait_recv()
    for way in range(2):
        wb_copy(way, 3).start()
    wd_copy(0).start()
    w_forward(0)
    job = run(opposite(2, 3), (0,), (1,), job)
    d_arrived((2, 3), (3, 3))
    job = run(opposite(2, 3), (1,), (1,), job)
    flush(job)

    def result(r):
        done = acc[r] / ls[r]
        return [jnp.transpose(done[:, i * 128:(i + 1) * 128]).astype(jnp.bfloat16) for i in range(4)]

    for i, part in enumerate(result(1)):
        osend[:, i * 128:(i + 1) * 128] = part
    o_copy = remote(osend, att.at[g], o_s, o_r, pair)
    o_copy.start()
    w_forward(1)
    job = run(side(3), (0, 1), (0,))
    w_forward(2)
    flush(run(opposite(0, 1, 2, 3), (0, 1), (0,), job))
    for i, part in enumerate(result(0)):
        att[g, :, i * 128:(i + 1) * 128] = part
    wcopy.wait()
    o_copy.wait()

    x_copy = remote(att.at[:, pl.ds(pl.multiple_of((1 - h) * 64, 64), 64)], attx, x_s, x_r, across)
    x_copy.start()
    w_forward(3)
    for j in range(4):
        wb_copy((1, 1, 0, 0)[j], j).wait_recv()
    wd_copy(1).start()
    wd_copy(2).start()
    mine = [jnp.where(h == 0, att[i, 0:64], att[i, 64:128]) for i in range(2)]

    def project(n, carry):
        at = cols(n * COLS, COLS)
        part = jnp.dot(mine[0], w[0:512, at], preferred_element_type=jnp.float32)
        tot[:, at] = part + jnp.dot(mine[1], w[512:1024, at], preferred_element_type=jnp.float32)
        return carry

    lax.fori_loop(0, 4096 // COLS, project, 0)

    for j in range(3):
        wg_copy(j).wait_recv()
        wh_copy(j).start()
    x_copy.wait()

    def share(i, at):
        left, right = [], []
        for st in range(2):
            base = b * (1 - c) + a * c if st == 0 else b * c + a * (1 - c)
            bb = unit_of(base, i)
            left.append(attx[st, :, cols(bb * 128, 128)])
            right.append(wo[st, bb, :, :, at].reshape(128, COLS))
        return jnp.dot(jnp.concatenate(left, axis=1), jnp.concatenate(right, axis=0),
                       preferred_element_type=jnp.float32)

    for i in range(3):
        wd_copy(i).wait_recv()

    def project_near(n, carry):
        at = cols(n * COLS, COLS)
        tot[:, at] = tot[:, at] + (share(0, at) + share(1, at) + share(2, at))
        return carry

    lax.fori_loop(0, 4096 // COLS, project_near, 0)
    wg_copy(3).wait_recv()
    wh_copy(3).start()
    for j in range(4):
        wh_copy(j).wait_recv()

    def project_far(n, carry):
        at = cols(n * COLS, COLS)
        out_ref[:, at] = (tot[:, at] + share(3, at)).astype(jnp.bfloat16)
        return carry

    lax.fori_loop(0, 4096 // COLS, project_far, 0)

    def drain(k, carry):
        for way in range(3):
            a_copy(k, way).wait_send()
        for way in range(4):
            b_copy(k, way).wait_send()
        for i in range(4):
            d_copy(k, i).wait_send()
        return carry

    lax.fori_loop(0, 4, drain, 0)
    for k in (1, 2, 3):
        for t in range(2):
            z_copy(k, t).wait_send()
    for way in range(2):
        wf_copy(way).wait_send()
        wa_copy(way).wait_send()
        for j in range(4):
            wb_copy(way, j).wait_send()
    for i in range(3):
        wd_copy(i).wait_send()
    for j in range(4):
        wg_copy(j).wait_send()
        wh_copy(j).wait_send()


def per_device(queries, keys, values, tile_mask, out_weight):
    dma = pltpu.SemaphoreType.DMA
    bf, f32 = jnp.bfloat16, jnp.float32
    return pl.pallas_call(
        kernel,
        out_shape=jax.ShapeDtypeStruct((64, 4096), bf),
        in_specs=[pl.BlockSpec(memory_space=pltpu.HBM)] * 5,
        out_specs=pl.BlockSpec(memory_space=pltpu.VMEM),
        scratch_shapes=[
            pltpu.VMEM((2, 4, 4, 2, 4, 128, 128), bf),
            pltpu.VMEM((2, 128, 256), bf),
            pltpu.VMEM((2, 4, 128, 128), bf),
            pltpu.VMEM((1024, 4096), bf),
            pltpu.VMEM((2, 4, 4, 32, 4096), bf),
            pltpu.VMEM((2, 8, 256), jnp.int32),
            pltpu.VMEM((2, 256, 1, 128), f32),
            pltpu.VMEM((2, 2, 1, 128), f32),
            pltpu.VMEM((2, 1, 512), f32),
            pltpu.VMEM((2, 1, 512), f32),
            pltpu.VMEM((2, 128, 512), f32),
            pltpu.VMEM((512, 512), f32),
            pltpu.VMEM((2, 128, 512), bf),
            pltpu.VMEM((2, 64, 512), bf),
            pltpu.VMEM((128, 512), bf),
            pltpu.VMEM((64, 4096), f32),
            dma((4,)), dma((4,)), dma, dma((2,)),
            dma((4, 2)), dma((4, 2)), dma((4,)), dma((4,)),
            dma((4, 3)), dma((4, 3)), dma((4, 4)), dma((4, 4)), dma((4, 4)), dma((4, 4)),
            dma, dma, dma((2,)), dma((2,)), dma((2,)), dma((2,)), dma((2, 4)), dma((2, 4)),
            dma((4,)), dma((4,)), dma((3,)), dma((3,)), dma((4,)), dma((4,)), dma, dma,
        ],
        compiler_params=pltpu.CompilerParams(
            collective_id=0, has_side_effects=True, vmem_limit_bytes=67043328),
    )(queries, keys, values, tile_mask, out_weight)


def solution(mesh):
    placed = (P("seq", "head"), P("seq", "head"), P("seq", "head"), P(), P("head", None))
    return jax.shard_map(
        per_device, mesh=mesh, in_specs=placed, out_specs=P(("seq", "head"), None), check_vma=False
    )
```

```python
import math

import jax
import jax.numpy as jnp
from jax import lax
from jax.experimental import pallas as pl
from jax.experimental.pallas import tpu as pltpu
from jax.sharding import PartitionSpec as P

HD = 128
MESH = pl.DeviceIdType.MESH
OFF = -1e30
FLOOR = -1e6
EXP_SCALE = math.log2(math.e) / math.sqrt(HD)
COLS = 512


def kernel(q_hbm, k_hbm, v_hbm, mask_hbm, w_hbm, out_ref,
           buf, kv, qs, w, wo, mask8, bias, dbias, mx, ls, acc, sbuf, att, attx, osend, tot,
           lsem, qlsem, wsem, msem, zs, zr, qss, qsr, a_s, a_r, b_s, b_r, d_s, d_r, o_s, o_r,
           wf_s, wf_r, wa_s, wa_r, wb_s, wb_r, wg_s, wg_r, wd_s, wd_r, wh_s, wh_r, x_s, x_r):
    s = lax.axis_index("seq")
    h = lax.axis_index("head")
    c = s % 2
    y = (s // 2) % 4
    z = (s // 8) % 4
    x = s // 32
    a = y * (1 - c) + x * c
    b = x * (1 - c) + y * c
    g = z % 2
    chip = x * 16 + z * 4 + y
    pair_z = z + 1 - 2 * g
    pair_chip = (3 - x) * 16 + pair_z * 4 + y

    def dev(xx, zz, yy, cc, hh):
        return {"seq": ((xx * 4 + zz) * 4 + yy) * 2 + cc, "head": hh}

    def a_dev(d):
        return dev((x + c * d + 4) % 4, z, (y + (1 - c) * d + 4) % 4, c, h)

    def b_dev(d):
        return dev((x + (1 - c) * d + 4) % 4, z, (y + c * d + 4) % 4, c, h)

    def z_of(k):
        return ((z // 2 + k // 2) % 2) * 2 + (z % 2 + k % 2) % 2

    mate = dev(x, z, y, 1 - c, h)
    pair = dev(3 - x, pair_z, y, c, h)
    across = dev(x, z, y, c, 1 - h)

    def remote(src, dst, ss, rs, to):
        return pltpu.make_async_remote_copy(
            src_ref=src, dst_ref=dst, send_sem=ss, recv_sem=rs, device_id=to, device_id_type=MESH)

    def cols(start, size):
        return pl.ds(pl.multiple_of(start, 128), size)

    locals_ = [
        pltpu.make_async_copy(k_hbm.at[:, cols(g * 128, 128)], buf.at[c, b, z, 0, a], lsem.at[0]),
        pltpu.make_async_copy(v_hbm.at[:, cols(g * 128, 128)], buf.at[c, b, z, 1, a], lsem.at[1]),
    ]
    qlocals = [
        pltpu.make_async_copy(q_hbm.at[:, cols(g * 512 + i * 128, 128)], qs.at[0, i], qlsem.at[i])
        for i in range(4)
    ]
    mask_own = pltpu.make_async_copy(
        mask_hbm.at[pl.ds(pl.multiple_of((chip // 2) * 8, 8), 8)], mask8.at[0], msem.at[0])
    mask_pair = pltpu.make_async_copy(
        mask_hbm.at[pl.ds(pl.multiple_of((pair_chip // 2) * 8, 8), 8)], mask8.at[1], msem.at[1])
    stage = [pltpu.make_async_copy(k_hbm, kv.at[0], lsem.at[2]), pltpu.make_async_copy(v_hbm, kv.at[1], lsem.at[3])]
    for cp in stage + locals_:
        cp.start()

    barrier = pltpu.get_barrier_semaphore()
    friends = [a_dev(1), a_dev(-1), a_dev(2), b_dev(1), b_dev(-1), mate, pair, across] + [
        dev(x, z_of(k), y, c, h) for k in (1, 2, 3)]
    for f in friends:
        pl.semaphore_signal(barrier, inc=1, device_id=f, device_id_type=MESH)
    mask_own.start()
    mask_pair.start()
    for cp in qlocals:
        cp.start()
    pl.semaphore_wait(barrier, len(friends))

    def z_copy(k, t):
        zt = z_of(k)
        return remote(kv.at[t, :, cols((zt % 2) * 128, 128)], buf.at[c, b, z, t, a],
                      zs.at[k, t], zr.at[k, t], dev(x, zt, y, c, h))

    def q_copy(i):
        return remote(q_hbm.at[:, cols((1 - g) * 512 + i * 128, 128)], qs.at[1, i],
                      qss.at[i], qsr.at[i], pair)

    def a_copy(k, way):
        zt = z_of(k)
        if way == 0:
            ref, to = buf.at[c, b, zt, :, a], a_dev(1)
        elif way == 1:
            ref, to = buf.at[c, b, zt, :, a], a_dev(-1)
        else:
            ref, to = buf.at[c, b, zt, :, a], a_dev(2)
        return remote(ref, ref, a_s.at[k, way], a_r.at[k, way], to)

    def b_copy(k, way):
        zt = z_of(k)
        if way == 0:
            ref, to = buf.at[c, b, zt], b_dev(1)
        elif way == 1:
            ref, to = buf.at[c, b, zt], b_dev(-1)
        elif way == 2:
            ref, to = buf.at[c, (b + 3) % 4, zt, 0], b_dev(1)
        else:
            ref, to = buf.at[c, (b + 1) % 4, zt, 1], b_dev(-1)
        return remote(ref, ref, b_s.at[k, way], b_r.at[k, way], to)

    def unit_of(base, i):
        return (base + (4 - i) * (i % 2) * (1 - i // 2) + (i // 2) * (1 + i % 2)) % 4

    def d_copy(k, i):
        ref = buf.at[c, unit_of(b, i), z_of(k)]
        return remote(ref, ref, d_s.at[k, i], d_r.at[k, i], mate)

    def wf_copy(i):
        slot = (a + 2 * i) % 4
        row = pl.multiple_of(((c * 4 + b) * 4 + slot) * 32, 32)
        return remote(w_hbm.at[pl.ds(row, 32)], wo.at[c, b, slot], wf_s.at[i], wf_r.at[i], across)

    def wa_copy(way):
        ref = wo.at[c, b, a]
        return remote(ref, ref, wa_s.at[way], wa_r.at[way], a_dev(1 - 2 * way))

    def slot_of(j):
        return (a + (0, 3, 1, 2)[j]) % 4

    def wb_copy(way, j):
        ref = wo.at[c, b, slot_of(j)]
        return remote(ref, ref, wb_s.at[way, j], wb_r.at[way, j], b_dev(1 - 2 * way))

    def wg_copy(j):
        ref = wo.at[c, (b + (3, 3, 1, 1)[j]) % 4, slot_of(j)]
        return remote(ref, ref, wg_s.at[j], wg_r.at[j], b_dev((1, 1, -1, -1)[j]))

    def wh_copy(j):
        ref = wo.at[c, (b + 2) % 4, slot_of(j)]
        return remote(ref, ref, wh_s.at[j], wh_r.at[j], mate)

    def w_forward(j):
        wb_copy((0, 0, 1, 1)[j], j).wait_recv()
        wg_copy(j).start()

    def wd_copy(i):
        ref = wo.at[c, unit_of(b, i)]
        return remote(ref, ref, wd_s.at[i], wd_r.at[i], mate)

    for cp in stage:
        cp.wait()
    for k in (1, 2, 3):
        for t in range(2):
            z_copy(k, t).start()
    for i in range(4):
        q_copy(i).start()
    wf_copy(0).start()
    for cp in locals_:
        cp.wait()
    for way in range(3):
        a_copy(0, way).start()
    wcopy = pltpu.make_async_copy(w_hbm, w, wsem)
    wcopy.start()

    mask_own.wait()
    mask_pair.wait()
    for r, row_chip in ((0, chip), (1, pair_chip)):
        at = (row_chip % 2) * 2 + c
        all8 = mask8[r]
        two = jnp.where(at < 2, jnp.where(at == 0, all8[0:2], all8[2:4]),
                        jnp.where(at == 2, all8[4:6], all8[6:8]))
        open2 = jnp.where(two > 0, 0.0, OFF).astype(jnp.float32)
        wide = jnp.concatenate([jnp.broadcast_to(open2[i:i + 1], (64, 256)) for i in range(2)], axis=0)
        bias[r] = jnp.transpose(wide).reshape(256, 1, 128)
        for i in range(2):
            own_tile = (row_chip * 2 + c) * 2 + i
            dbias[r, i] = bias[r, own_tile]
            bias[r, own_tile] = jnp.full((1, 128), OFF, jnp.float32)

    mx[...] = jnp.full(mx.shape, FLOOR, jnp.float32)
    ls[...] = jnp.zeros(ls.shape, jnp.float32)
    acc[...] = jnp.zeros(acc.shape, jnp.float32)

    def masked(scores, r, rows):
        tiles = [jnp.broadcast_to(jnp.concatenate([row] * 4, axis=1), (64, 512)) for row in rows]
        return scores + jnp.concatenate(tiles, axis=0)

    def dot_keys(keys, r):
        return lax.dot_general(keys, qs[r].reshape(512, HD), (((1,), (1,)), ((), ())),
                               preferred_element_type=jnp.float32)

    def soften(r, scores, best):
        old = mx[r]
        new = jnp.maximum(old, best)
        probs = jnp.exp2((scores - new) * EXP_SCALE)
        shrink = jnp.exp2((old - new) * EXP_SCALE)
        ls[r] = ls[r] * shrink + jnp.sum(probs, axis=0, keepdims=True)
        mx[r] = new
        return probs.astype(jnp.bfloat16), shrink

    def blend(r, probs, shrink, vals):
        acc[r] = acc[r] * shrink + lax.dot_general(
            vals, probs, (((0,), (0,)), ((), ())), preferred_element_type=jnp.float32)

    def first_chip(st, bb, zz):
        return (1 - st) * (bb * 16 + zz * 4) + st * (zz * 4 + bb)

    def score_job(job):
        st, halves, r = job[0], ((job[1], job[2], 0), (job[3], job[4], job[5])), job[6]
        rows, keys = [], []
        for bb, zz, first in halves:
            keys.append(buf[st, bb, zz, 0, pl.ds(first, 2)].reshape(256, HD))
            for i in range(2):
                tile = (((1 - st) * (bb * 16 + zz * 4 + first + i)
                         + st * ((first + i) * 16 + zz * 4 + bb)) * 2 + st) * 2
                rows += [bias[r, tile], bias[r, tile + 1]]
        scores = masked(dot_keys(jnp.concatenate(keys, axis=0), r), r, rows)
        sbuf[...] = scores
        return jnp.max(scores, axis=0, keepdims=True)

    def weigh_job(job):
        return soften(job[6], sbuf[...], job[7])

    def blend_job(job, probs, shrink):
        st = job[0]
        vals = [buf[st, job[1], job[2], 1, 0:2].reshape(256, HD),
                buf[st, job[3], job[4], 1, pl.ds(job[5], 2)].reshape(256, HD)]
        blend(job[6], probs, shrink, jnp.concatenate(vals, axis=0))

    def flush(job):
        probs, shrink = weigh_job(job)
        blend_job(job, probs, shrink)

    def pick(values, at):
        out = values[0]
        for i in range(1, len(values)):
            out = jnp.where(at == i, values[i], out)
        return out

    def run(units, streams, rows, pending=None):
        count = len(units) * len(streams) * len(rows)

        def parts(n):
            u = n % len(units)
            r = pick(rows, (n // len(units)) % len(rows))
            other = pick(streams, n // len(units) // len(rows))
            st = c * (1 - other) + (1 - c) * other
            early = 1 - (x * (1 - r) + (3 - x) * r) // 2
            base = b * (1 - other) + a * other

            def place(v):
                return unit_of(base, pick([i for _, i in units], v)), z_of(pick([k for k, _ in units], v))

            here = place(u)
            there = place(u - u % 2 + 1)
            return st, u % 2, here, there, r, st * early

        def job_at(n):
            st, _, here, there, r, joined = parts(n)
            return (st, here[0], here[1], here[0] * (1 - joined) + there[0] * joined,
                    here[1] * (1 - joined) + there[1] * joined, 2 * (1 - joined), r)

        ends, total = [], 0
        for n in range(count):
            st, odd, here, there, r, joined = parts(n)
            row_chip = chip * (1 - r) + pair_chip * r
            mine = jnp.where(first_chip(st, *here) <= row_chip, 1, 0)
            other_one = jnp.where(first_chip(st, *there) <= row_chip, 1, 0)
            use = mine * (1 - joined) + joined * (1 - odd) * jnp.maximum(mine, other_one)
            total = total + use
            ends.append(total)

        def nth(t):
            n = 0
            for end in ends[:-1]:
                n = n + jnp.where(end <= t, 1, 0)
            return tuple(jnp.asarray(v, jnp.int32) for v in job_at(n))

        def body(t, job):
            probs, shrink = weigh_job(job)
            following = nth(t)
            best = score_job(following)
            blend_job(job, probs, shrink)
            return following + (best,)

        if pending is not None:
            return lax.fori_loop(0, total, body, pending)
        start = nth(0)
        return lax.fori_loop(1, total, body, start + (score_job(start),))

    def diagonal(r, carry):
        zz = z * (1 - r) + pair_z * r
        xx = x * (1 - r) + (3 - x) * r
        aa = y * (1 - c) + xx * c
        bb = xx * (1 - c) + y * c
        scores = masked(dot_keys(buf[c, bb, zz, 0, aa], r), r, [dbias[r, 0], dbias[r, 1]])
        key = lax.broadcasted_iota(jnp.int32, (128, 512), 0)
        row = lax.broadcasted_iota(jnp.int32, (128, 512), 1) % 128
        scores = jnp.where(key <= row, scores, OFF)
        probs, shrink = soften(r, scores, jnp.max(scores, axis=0, keepdims=True))
        blend(r, probs, shrink, buf[c, bb, zz, 1, aa])
        return carry

    def a_begin(k):
        z_copy(k, 0).wait_recv()
        z_copy(k, 1).wait_recv()
        for way in range(3):
            a_copy(k, way).start()

    def b_begin(k):
        for way in range(3):
            a_copy(k, way).wait_recv()
        b_copy(k, 0).start()
        b_copy(k, 1).start()
        d_copy(k, 0).start()

    def d_arrived(*pairs):
        for k, i in pairs:
            d_copy(k, i).wait_recv()

    def near(k):
        b_copy(k, 0).wait_recv()
        b_copy(k, 2).start()
        b_copy(k, 1).wait_recv()
        b_copy(k, 3).start()
        d_copy(k, 1).start()
        d_copy(k, 2).start()

    def far(k):
        b_copy(k, 2).wait_recv()
        b_copy(k, 3).wait_recv()
        d_copy(k, 3).start()

    def own(*ks):
        return tuple((k, 0) for k in ks)

    def side(k):
        return ((k, 1), (k, 2))

    def opposite(*ks):
        return tuple((k, 3) for k in ks)

    a_begin(1)
    b_begin(0)
    a_begin(2)
    a_begin(3)
    for cp in qlocals:
        cp.wait()
    diagonal(0, 0)
    for i in range(4):
        q_copy(i).wait()
    b_begin(1)
    job = run(own(0, 1), (0,), (0, 1))
    b_begin(2)
    b_begin(3)
    d_arrived((0, 0), (1, 0))
    job = run(own(0, 1), (1,), (0, 1), job)
    near(0)
    wf_copy(1).start()
    job = run(own(2, 3), (0,), (0, 1), job)
    near(1)
    d_arrived((2, 0), (3, 0))
    job = run(own(2, 3), (1,), (0, 1), job)
    near(2)
    d_arrived((0, 1), (0, 2))
    job = run(side(0), (0, 1), (1,), job)
    near(3)
    wf_copy(0).wait_recv()
    for way in range(2):
        wa_copy(way).start()
        wb_copy(way, 0).start()
    diagonal(1, 0)
    d_arrived((1, 1), (1, 2))
    job = run(side(1), (0, 1), (1,), job)
    job = run(side(0), (0, 1), (0,), job)
    far(0)
    d_arrived((2, 1), (2, 2))
    job = run(side(2), (0, 1), (1,), job)
    far(1)
    d_arrived((3, 1), (3, 2))
    job = run(side(3), (0, 1), (1,), job)
    job = run(side(1), (0, 1), (0,), job)
    far(2)
    for way in range(2):
        wa_copy(way).wait_recv()
    for j in (1, 2):
        for way in range(2):
            wb_copy(way, j).start()
    d_arrived((0, 3), (1, 3))
    job = run(opposite(0, 1), (0, 1), (1,), job)
    job = run(side(2), (0, 1), (0,), job)
    far(3)
    wf_copy(1).wait_recv()
    for way in range(2):
        wb_copy(way, 3).start()
    wd_copy(0).start()
    w_forward(0)
    job = run(opposite(2, 3), (0,), (1,), job)
    d_arrived((2, 3), (3, 3))
    job = run(opposite(2, 3), (1,), (1,), job)
    flush(job)

    def result(r):
        done = acc[r] / ls[r]
        return [jnp.transpose(done[:, i * 128:(i + 1) * 128]).astype(jnp.bfloat16) for i in range(4)]

    for i, part in enumerate(result(1)):
        osend[:, i * 128:(i + 1) * 128] = part
    o_copy = remote(osend, att.at[g], o_s, o_r, pair)
    o_copy.start()
    job = run(side(3), (0, 1), (0,))
    flush(run(opposite(0, 1, 2, 3), (0, 1), (0,), job))
    for i, part in enumerate(result(0)):
        att[g, :, i * 128:(i + 1) * 128] = part
    wcopy.wait()
    o_copy.wait()

    x_copy = remote(att.at[:, pl.ds(pl.multiple_of((1 - h) * 64, 64), 64)], attx, x_s, x_r, across)
    x_copy.start()
    w_forward(1)
    w_forward(2)
    w_forward(3)
    for j in range(4):
        wb_copy((1, 1, 0, 0)[j], j).wait_recv()
    wd_copy(1).start()
    wd_copy(2).start()
    mine = [jnp.where(h == 0, att[i, 0:64], att[i, 64:128]) for i in range(2)]

    def project(n, carry):
        at = cols(n * COLS, COLS)
        part = jnp.dot(mine[0], w[0:512, at], preferred_element_type=jnp.float32)
        tot[:, at] = part + jnp.dot(mine[1], w[512:1024, at], preferred_element_type=jnp.float32)
        return carry

    lax.fori_loop(0, 4096 // COLS, project, 0)

    for j in range(3):
        wg_copy(j).wait_recv()
        wh_copy(j).start()
    x_copy.wait()

    def share(i, at):
        left, right = [], []
        for st in range(2):
            base = b * (1 - c) + a * c if st == 0 else b * c + a * (1 - c)
            bb = unit_of(base, i)
            left.append(attx[st, :, cols(bb * 128, 128)])
            right.append(wo[st, bb, :, :, at].reshape(128, COLS))
        return jnp.dot(jnp.concatenate(left, axis=1), jnp.concatenate(right, axis=0),
                       preferred_element_type=jnp.float32)

    for i in range(3):
        wd_copy(i).wait_recv()

    def project_near(n, carry):
        at = cols(n * COLS, COLS)
        tot[:, at] = tot[:, at] + (share(0, at) + share(1, at) + share(2, at))
        return carry

    lax.fori_loop(0, 4096 // COLS, project_near, 0)
    wg_copy(3).wait_recv()
    wh_copy(3).start()
    for j in range(4):
        wh_copy(j).wait_recv()

    def project_far(n, carry):
        at = cols(n * COLS, COLS)
        out_ref[:, at] = (tot[:, at] + share(3, at)).astype(jnp.bfloat16)
        return carry

    lax.fori_loop(0, 4096 // COLS, project_far, 0)

    def drain(k, carry):
        for way in range(3):
            a_copy(k, way).wait_send()
        for way in range(4):
            b_copy(k, way).wait_send()
        for i in range(4):
            d_copy(k, i).wait_send()
        return carry

    lax.fori_loop(0, 4, drain, 0)
    for k in (1, 2, 3):
        for t in range(2):
            z_copy(k, t).wait_send()
    for way in range(2):
        wf_copy(way).wait_send()
        wa_copy(way).wait_send()
        for j in range(4):
            wb_copy(way, j).wait_send()
    for i in range(3):
        wd_copy(i).wait_send()
    for j in range(4):
        wg_copy(j).wait_send()
        wh_copy(j).wait_send()


def per_device(queries, keys, values, tile_mask, out_weight):
    dma = pltpu.SemaphoreType.DMA
    bf, f32 = jnp.bfloat16, jnp.float32
    return pl.pallas_call(
        kernel,
        out_shape=jax.ShapeDtypeStruct((64, 4096), bf),
        in_specs=[pl.BlockSpec(memory_space=pltpu.HBM)] * 5,
        out_specs=pl.BlockSpec(memory_space=pltpu.VMEM),
        scratch_shapes=[
            pltpu.VMEM((2, 4, 4, 2, 4, 128, 128), bf),
            pltpu.VMEM((2, 128, 256), bf),
            pltpu.VMEM((2, 4, 128, 128), bf),
            pltpu.VMEM((1024, 4096), bf),
            pltpu.VMEM((2, 4, 4, 32, 4096), bf),
            pltpu.VMEM((2, 8, 256), jnp.int32),
            pltpu.VMEM((2, 256, 1, 128), f32),
            pltpu.VMEM((2, 2, 1, 128), f32),
            pltpu.VMEM((2, 1, 512), f32),
            pltpu.VMEM((2, 1, 512), f32),
            pltpu.VMEM((2, 128, 512), f32),
            pltpu.VMEM((512, 512), f32),
            pltpu.VMEM((2, 128, 512), bf),
            pltpu.VMEM((2, 64, 512), bf),
            pltpu.VMEM((128, 512), bf),
            pltpu.VMEM((64, 4096), f32),
            dma((4,)), dma((4,)), dma, dma((2,)),
            dma((4, 2)), dma((4, 2)), dma((4,)), dma((4,)),
            dma((4, 3)), dma((4, 3)), dma((4, 4)), dma((4, 4)), dma((4, 4)), dma((4, 4)),
            dma, dma, dma((2,)), dma((2,)), dma((2,)), dma((2,)), dma((2, 4)), dma((2, 4)),
            dma((4,)), dma((4,)), dma((3,)), dma((3,)), dma((4,)), dma((4,)), dma, dma,
        ],
        compiler_params=pltpu.CompilerParams(
            collective_id=0, has_side_effects=True, vmem_limit_bytes=67043328),
    )(queries, keys, values, tile_mask, out_weight)


def solution(mesh):
    placed = (P("seq", "head"), P("seq", "head"), P("seq", "head"), P(), P("head", None))
    return jax.shard_map(
        per_device, mesh=mesh, in_specs=placed, out_specs=P(("seq", "head"), None), check_vma=False
    )
```
